32 devices in a mesh: band: 4 (over x, core), grid: 8 (over z, y).
Axes of the slice: x: 2, y: 2, z: 4, core: 2. Of those that a mesh axis runs over, the one named last changes fastest.
Arguments:
- orbitals: float32 [8, 128, 128, 128], P('band', 'grid'), may hold values from -6 to 6
- occupation: float32 [8], P('band'), may hold values from 0.25 to 1
- g_list: int32 [131072], P('grid'), may hold values from 0 to 262143, as said below
- positions: float32 [3, 512], replicated, may hold values from 0 to 1
- species: int32 [512], replicated, may hold values from 0 to 3
- widths: float32 [4], replicated, may hold values from 0.3 to 2
Outputs:
- stress: float32 [3, 3], replicated
- atom_terms: float32 [512], replicated
The draws below stay inside these ranges and needn't reach their ends.
Inputs may be any that keep to these rules, and one draw needn't show every extreme that they name: `g_list`: within each aligned block of 16384 entries the values are distinct and increasing.
All inputs are finite; a program needn't handle non-finite values.
Results may differ from the reference program's by a relative error of at most 0.00013.
Values sent between devices are 32-bit elements; how exact they have to be, the bound alone decides.
A program may use at most 64 MiB of HBM per device.

```python
import math
import jax
import jax.numpy as jnp
from jax import lax

NX = 128
NY = 128
NZ = 128
GSEL_DEV = 16384
ATOMS = 512
SPECIES = 4
NBANDS = 8
SLAB_Y = 16
N_GRID = 8


def draw_orbitals(key, part):
    key_noise = jax.random.fold_in(key, 11)
    key_amplitude = jax.random.fold_in(key, 12)
    key_modes = jax.random.fold_in(key, 13)
    key_offset = jax.random.fold_in(key, 14)
    key_filter = jax.random.fold_in(key, 16)
    key_envelope = jax.random.fold_in(key, 17)
    shape = (NBANDS, NX, NY, NZ)
    noise_part = 0.3 * jnp.clip(jax.random.normal(key_noise, shape, jnp.float32), -4.0, 4.0)
    strength = jax.random.uniform(key_filter, (NBANDS,), jnp.float32, 0.04, 0.12)
    swing = jax.random.uniform(jax.random.fold_in(key_envelope, 1), (NBANDS,), jnp.float32, 0.1, 0.3)
    amp_low = 0.3
    amp_high = 0.55
    beside = jnp.roll(noise_part, 1, axis=1) + jnp.roll(noise_part, -1, axis=1)
    beside = beside + jnp.roll(noise_part, 1, axis=2) + jnp.roll(noise_part, -1, axis=2)
    beside = beside + jnp.roll(noise_part, 1, axis=3) + jnp.roll(noise_part, -1, axis=3)
    colored = noise_part + strength[:, None, None, None] * beside
    axis_x = jnp.arange(NX, dtype=jnp.float32)[None, :, None, None] / NX
    axis_y = jnp.arange(NY, dtype=jnp.float32)[None, None, :, None] / NY
    axis_z = jnp.arange(NZ, dtype=jnp.float32)[None, None, None, :] / NZ
    low_x = jax.random.randint(jax.random.fold_in(key_envelope, 2), (NBANDS,), -2, 3).astype(jnp.float32)
    low_y = jax.random.randint(jax.random.fold_in(key_envelope, 3), (NBANDS,), -2, 3).astype(jnp.float32)
    low_z = jax.random.randint(jax.random.fold_in(key_envelope, 4), (NBANDS,), -2, 3).astype(jnp.float32)
    low_phase = jax.random.uniform(jax.random.fold_in(key_envelope, 5), (NBANDS,), jnp.float32, -math.pi, math.pi)
    envelope_angle = 2.0 * math.pi * (low_x[:, None, None, None] * axis_x + low_y[:, None, None, None] * axis_y + low_z[:, None, None, None] * axis_z) + low_phase[:, None, None, None]
    envelope = 1.0 + swing[:, None, None, None] * jnp.cos(envelope_angle)
    start = (envelope * colored).astype(jnp.float32)

    def add_wave(wave, result):
        wave_key = jax.random.fold_in(key_modes, wave)
        mode_x = jax.random.randint(jax.random.fold_in(wave_key, 1), (NBANDS,), -(NX // 2), NX // 2).astype(jnp.float32)
        mode_y = jax.random.randint(jax.random.fold_in(wave_key, 2), (NBANDS,), -(NY // 2), NY // 2).astype(jnp.float32)
        mode_z = jax.random.randint(jax.random.fold_in(wave_key, 3), (NBANDS,), -(NZ // 2), NZ // 2).astype(jnp.float32)
        offset = jax.random.uniform(jax.random.fold_in(key_offset, wave), (NBANDS,), jnp.float32, -math.pi, math.pi)
        amplitude = jax.random.uniform(jax.random.fold_in(key_amplitude, wave), (NBANDS,), jnp.float32, amp_low, amp_high)
        angles = 2.0 * math.pi * (mode_x[:, None, None, None] * axis_x + mode_y[:, None, None, None] * axis_y + mode_z[:, None, None, None] * axis_z) + offset[:, None, None, None]
        return result + amplitude[:, None, None, None] * jnp.cos(angles)
    result = lax.fori_loop(0, 48, add_wave, start)
    return jnp.clip(result, -6.0, 6.0)


def draw_g_list(key, part):
    local_cells = NX * SLAB_Y * NZ
    slab_keys = jax.random.split(jax.random.fold_in(key, 21), N_GRID)

    def one_slab(slab_key):
        return jnp.sort(jax.random.permutation(slab_key, local_cells)[:GSEL_DEV])
    return jax.vmap(one_slab)(slab_keys).reshape(-1).astype(jnp.int32)


def touch_ends(values, stream_key, smallest, largest):
    longest = values.shape.index(max(values.shape))
    spots = []
    for shift in (0, 1):
        where = [jax.random.randint(jax.random.fold_in(stream_key, axis), (), 0, length) for axis, length in enumerate(values.shape)]
        where[longest] = (where[longest] + shift) % values.shape[longest]
        spots.append(tuple(where))
    return values.at[spots[0]].set(smallest).at[spots[1]].set(largest)


def shard_levels(key, extent, pieces, low, high):
    gain, own = 1.0, jax.random.fold_in(key, 6)
    for position, blocks in pieces:
        steps = jnp.exp(jax.random.uniform(jax.random.fold_in(own, position), (blocks,), jnp.float32, low / len(pieces), high / len(pieces)))
        gain = gain * jnp.repeat(steps, extent[position] // blocks).reshape([-1 if axis == position else 1 for axis in range(len(extent))])
    return gain


def setup_inputs(seed: int = 0) -> dict:
    splits = jax.random.split(jax.random.key(seed), 7)
    return {
        "orbitals": draw_orbitals(jax.random.fold_in(splits[6], 71), 0),
        "occupation": jnp.clip(0.25 + 0.75 * jax.random.uniform(splits[1], (NBANDS,), jnp.float32) ** shard_levels(splits[1], (NBANDS,), ((0, 4),), -0.2, 0.2), 0.25, 1.0),
        "g_list": draw_g_list(jax.random.fold_in(splits[6], 71), 0),
        "positions": jnp.clip(jax.random.uniform(splits[3], (3, ATOMS), jnp.float32, 0.0, 1.0), 0.0, 1.0),
        "species": touch_ends(jax.random.randint(splits[4], (ATOMS,), 0, SPECIES), jax.random.fold_in(splits[4], 1), 0, SPECIES - 1).astype(jnp.int32),
        "widths": jnp.clip(jnp.exp(jax.random.uniform(splits[5], (SPECIES,), jnp.float32, math.log(0.3), math.log(2.0))), 0.3, 2.0),
    }


HIGHEST = lax.Precision.HIGHEST


def folded_frequency(cell, length):
    folded = jnp.where(cell < length // 2, cell, cell - length)
    return folded.astype(jnp.float32)


def spectrum_sums(selected, freq_x, freq_y, freq_z, positions, species, widths, lengths, band_total):
    two_pi = 2.0 * math.pi
    wave_vector = jnp.stack([two_pi * freq_x / lengths[0], two_pi * freq_y / lengths[1], two_pi * freq_z / lengths[2]])
    wave_square = jnp.sum(wave_vector * wave_vector, axis=0)
    nonzero = (wave_square > 0).astype(jnp.float32)
    denominator = wave_square + 1.0 - nonzero
    weighted = selected * (4.0 * math.pi) * nonzero / denominator
    identity = jnp.eye(3, dtype=jnp.float32)[:, :, None]
    kernel = 2.0 * wave_vector[:, None, :] * wave_vector[None, :, :] / denominator - identity
    stress = jnp.sum(kernel * weighted[None, None, :], axis=2) / band_total
    form_factor = jnp.exp(-0.5 * wave_square[None, :] * (widths * widths)[:, None]) * weighted[None, :]
    kinds = widths.shape[0]
    one_hot = (species[:, None] == jnp.arange(kinds, dtype=jnp.int32)[None, :]).astype(jnp.float32)
    atom_count = species.shape[0]
    fractions = positions.reshape(3, atom_count // 32, 32).transpose(1, 0, 2)
    hot_rows = one_hot.reshape(atom_count // 32, 32, kinds)

    def atom_block(operands):
        fraction, hot_block = operands
        phases = two_pi * (fraction[0][:, None] * freq_x[None, :] + fraction[1][:, None] * freq_y[None, :] + fraction[2][:, None] * freq_z[None, :])
        projected = jnp.dot(jnp.cos(phases), form_factor.T, precision=HIGHEST)
        return jnp.sum(projected * hot_block, axis=1)

    atom_terms = lax.map(atom_block, (fractions, hot_rows)).reshape(atom_count) / band_total
    return stress, atom_terms


def reference(orbitals, occupation, g_list, positions, species, widths):
    cells = NX * NY * NZ

    def add_band(accumulated, operands):
        orbital_row, occupied = operands
        pair_rows = orbital_row[None] * orbitals
        spectra = jnp.fft.fftn(pair_rows, axes=(1, 2, 3)) / cells
        pair_power = jnp.real(spectra) ** 2 + jnp.imag(spectra) ** 2
        weights = occupied * occupation
        return accumulated + jnp.einsum("p,pxyz->xyz", weights, pair_power, precision=HIGHEST), None

    spectrum, ignored = lax.scan(add_band, jnp.zeros((NX, NY, NZ), jnp.float32), (orbitals, occupation))
    entries = jnp.arange(g_list.shape[0], dtype=jnp.int32)
    slab_index = entries // GSEL_DEV
    cell_x = g_list // (SLAB_Y * NZ)
    cell_y = slab_index * SLAB_Y + (g_list // NZ) % SLAB_Y
    cell_z = g_list % NZ
    selected = spectrum[cell_x, cell_y, cell_z]
    return spectrum_sums(selected, folded_frequency(cell_x, NX), folded_frequency(cell_y, NY), folded_frequency(cell_z, NZ), positions, species, widths, (NX, NY, NZ), NBANDS)
```

```python
import functools
import math

import jax
import jax.numpy as jnp
import numpy as np
from jax import lax
from jax.experimental import pallas as pl
from jax.experimental.pallas import tpu as pltpu
from jax.sharding import PartitionSpec as P

HIGHEST = lax.Precision.HIGHEST
MESH = pl.DeviceIdType.MESH
TWO_PI = 2.0 * math.pi
F32 = jnp.float32
BF16 = jnp.bfloat16
CHUNK = 512
VMEM_LIMIT = 60 * 1024 * 1024

PAIRS = (
    (0, 0, 1.0), (0, 1, 2.0), (1, 1, 1.0), (0, 2, 2.0), (1, 3, 2.0),
    (0, 4, 2.0), (0, 5, 2.0), (1, 4, 2.0), (1, 5, 2.0),
)


def trig(rows, columns, length):
    angles = TWO_PI / length * (rows[:, None] * columns[None, :] % length)
    return np.cos(angles), np.sin(angles)


def halves(table):
    table = np.asarray(table, np.float32)
    high = table.astype(jnp.bfloat16)
    low = (table - high.astype(np.float32)).astype(jnp.bfloat16)
    return high, low


def split(value):
    high = value.astype(BF16)
    low = (value - high.astype(F32)).astype(BF16)
    return high, low


def dot(a, b):
    return jnp.dot(a, b, preferred_element_type=F32)


def select_kernel(
    count, depth, unroll, items, has_start,
    bands, item_chunk, item_row, orbitals, entries, basis_wide, basis_low, table_wide, table_low, turn, *rest,
):
    if has_start:
        start, out, planes, turned = rest
    else:
        out, planes, turned = rest
    slab_x, size_y, size_z = orbitals.shape[1:]
    rows = basis_low.shape[0] // 2
    width = count * 4 * depth
    half = slab_x // 2
    main = 4 * depth * 8

    @pl.when(pl.program_id(0) == 0)
    def transforms():
        if half < depth:
            planes[...] = jnp.zeros_like(planes)

        def one_pair(p, carry):
            left, right = bands[p, 0], bands[p, 1]
            origin = jnp.where(p < 8, p, main)
            pitch = jnp.where(p < 8, 8, 1)
            for block in range(half // unroll):
                parts = []
                for u in range(unroll):
                    up = half + block * unroll + u
                    down = half - 1 - block * unroll - u
                    above = orbitals[left, up] * orbitals[right, up]
                    below = orbitals[left, down] * orbitals[right, down]
                    parts += [above + below, above - below]
                high, low = split(jnp.concatenate(parts, axis=1))
                along = dot(basis_wide[...], jnp.concatenate([high, low], axis=0))
                along = along + dot(basis_low[...], high)
                stack = [along[:, i * size_z : (i + 1) * size_z] for i in range(2 * unroll)]
                high, low = split(jnp.concatenate(stack, axis=0))
                both = dot(jnp.concatenate([high, low], axis=1), table_wide[...])
                both = both + dot(high, table_low[...])
                for u in range(unroll):
                    for sign in range(2):
                        at = (2 * u + sign) * 2 * rows
                        cosine, sine = both[at : at + rows], both[at + rows : at + 2 * rows]
                        real = cosine[:, :size_z] - sine[:, size_z:]
                        imag = -(cosine[:, size_z:] + sine[:, :size_z])
                        for part, value in ((0, real), (1, imag)):
                            row = origin + ((2 * sign + part) * depth + block * unroll + u) * pitch
                            planes[pl.ds(row, rows, stride=width), :] = value
            return carry

        lax.fori_loop(0, count, one_pair, 0)

    chunks = entries.shape[0]
    base = pl.program_id(0) * items
    if has_start:
        out[...] = start[...]
    else:
        out[...] = jnp.zeros_like(out)

    def look_up(table, index):
        index = jnp.broadcast_to(index, table.shape)
        return jnp.take_along_axis(table, index, axis=1)

    steps = 4

    def prepare(i, carry):
        for u in range(steps):
            x_of = entries[i * steps + u, 1:2, :]
            turned[i * steps + u] = look_up(turn[...], x_of)
        return carry

    lax.fori_loop(0, chunks // steps, prepare, 0)

    def one_item(t):
        chunk, k = item_chunk[base + t], item_row[base + t]
        row_of = entries[chunk, 0:1, :]
        z_of = entries[chunk, 2:3, :]
        begin = pl.multiple_of(jnp.maximum(k, 0) * width, 8)
        around = turned.at[chunk]
        real = imag = None
        index = jnp.broadcast_to(z_of, (8, 128))
        get = lambda row: jnp.take_along_axis(planes[pl.ds(begin + row, 8), :], index, axis=1)
        for d in range(depth):
            cosine, sine = around[pl.ds(d, 1), :], around[pl.ds(depth + d, 1), :]
            picked = [get((part * depth + d) * 8) for part in range(4)]
            re = picked[0] * cosine + picked[3] * sine
            im = picked[1] * cosine - picked[2] * sine
            real, imag = (re, im) if real is None else (real + re, imag + im)
        last_real, last_imag = 0.0, 0.0
        for d in range(0, depth, 8):
            cosine, sine = around[pl.ds(d, 8), :], around[pl.ds(depth + d, 8), :]
            picked = [get(main + part * depth + d) for part in range(4)]
            last_real = last_real + jnp.sum(picked[0] * cosine + picked[3] * sine, axis=0, keepdims=True)
            last_imag = last_imag + jnp.sum(picked[1] * cosine - picked[2] * sine, axis=0, keepdims=True)
        here = row_of == k
        cosine = jnp.where(here, around[pl.ds(2 * depth, 1), :], 0.0)
        sine = jnp.where(here, around[pl.ds(2 * depth + 1, 1), :], 0.0)
        place = chunk // 4 * (count * 8) + chunk % 4
        for real, imag, first, many in ((real, imag, 0, 8), (last_real, last_imag, 64, 1)):
            for part, value in ((0, real * cosine + imag * sine), (1, imag * cosine - real * sine)):
                if many == 1:
                    where = pl.ds(place + 4 * part + first, 1)
                else:
                    where = pl.ds(place + 4 * part + first, many, stride=8)
                out[where, :] = out[where, :] + value

    def some_items(i, carry):
        for u in range(steps):
            one_item(i * steps + u)
        return carry

    lax.fori_loop(0, items // steps, some_items, 0)


def select(bands, item_chunk, item_row, orbitals, entries, slabs, tables, turn, start):
    count = len(PAIRS)
    slab_x, size_y, size_z = orbitals.shape[1:]
    half = slab_x // 2
    depth = -(-half // 8) * 8
    unroll = math.gcd(half, 4)
    chunks, fields, lanes = entries.shape
    block = chunks // slabs
    items = item_chunk.shape[0] // slabs
    rows = tables[1].shape[0] // 2
    whole = lambda a: pl.BlockSpec(a.shape, lambda i, *_: (0,) * a.ndim)
    moving = pl.BlockSpec((block * count * 2, 128), lambda i, *_: (i, 0))
    ins = [orbitals, entries, *tables, turn]
    specs = [whole(a) for a in ins]
    specs[1] = pl.BlockSpec((block, fields, lanes), lambda i, *_: (i, 0, 0))
    if start is not None:
        ins.append(start)
        specs.append(moving)
    return pl.pallas_call(
        functools.partial(select_kernel, count, depth, unroll, items, start is not None),
        out_shape=jax.ShapeDtypeStruct((chunks * count * 2, 128), F32),
        grid_spec=pltpu.PrefetchScalarGridSpec(
            num_scalar_prefetch=3,
            grid=(slabs,),
            in_specs=specs,
            out_specs=moving,
            scratch_shapes=[
                pltpu.VMEM((rows * count * 4 * depth, size_z), F32),
                pltpu.VMEM((block,) + turn.shape, F32),
            ],
        ),
        compiler_params=pltpu.CompilerParams(vmem_limit_bytes=VMEM_LIMIT),
        cost_estimate=pl.CostEstimate(
            flops=80_000_000_000, bytes_accessed=12_000_000, transcendentals=0
        ),
        name="select",
    )(bands, item_chunk, item_row, *ins)


def chain_kernel(
    pieces, share, height, weights,
    mine, out, inbox, power, heard, up_send, up_recv, down_send, down_recv, share_send, share_recv,
):
    band = lax.axis_index("band")
    grid = lax.axis_index("grid")
    bands, grids = lax.axis_size("band"), lax.axis_size("grid")
    links = grids // 2
    core, x = lax.rem(band, 2), lax.div(band, 2)
    mate, link = lax.rem(grid, 2), lax.div(grid, 2)
    groups = bands // 2 * 2
    family = groups * links
    my_class = x * 2 + mate

    def member(index):
        at_link, at_class = lax.div(index, groups), lax.rem(index, groups)
        return {"band": lax.div(at_class, 2) * 2 + core, "grid": at_link * 2 + lax.rem(at_class, 2)}

    me = link * groups + my_class
    barrier = pltpu.get_barrier_semaphore()

    def greet(step, carry):
        other = lax.rem(me + step, family)
        pl.semaphore_signal(barrier, inc=1, device_id=member(other), device_id_type=MESH)
        return carry

    lax.fori_loop(1, family, greet, 0)
    pl.semaphore_wait(barrier, family - 1)

    total = mine.shape[0]
    piece = total // 2 // pieces

    def hop(j, upward, source):
        at = pl.ds(pl.multiple_of(j * piece + (total // 2 if upward else 0), 8), piece)
        step = 1 if upward else -1
        return at, pltpu.make_async_remote_copy(
            src_ref=source.at[at],
            dst_ref=inbox.at[at],
            send_sem=(up_send if upward else down_send).at[j],
            recv_sem=(up_recv if upward else down_recv).at[j],
            device_id={"grid": lax.rem(grid + 2 * step + grids, grids)},
            device_id_type=MESH,
        )

    def begins(upward):
        return link == (0 if upward else links - 1)

    def ends(upward):
        return link == (links - 1 if upward else 0)

    def launch(j, carry):
        for upward in (True, False):
            @pl.when(begins(upward))
            def _():
                hop(j, upward, mine)[1].start()
        return carry

    lax.fori_loop(0, pieces, launch, 0)

    low = link < links // 2
    lag = 3

    def forward(step, carry):
        for upward in (True, False):
            j = step - jnp.where(low == upward, 0, lag)
            valid = jnp.logical_and(j >= 0, j < pieces)

            @pl.when(jnp.logical_and(valid, jnp.logical_not(begins(upward))))
            def _():
                at, copy = hop(j, upward, inbox)
                copy.wait_recv()
                inbox[at] = inbox[at] + mine[at]

                @pl.when(jnp.logical_not(ends(upward)))
                def _():
                    copy.start()

                @pl.when(ends(upward))
                def _():
                    chunks = piece // height
                    value = inbox[at].reshape(chunks, len(weights), height // len(weights), 128)
                    result = 0.0
                    for p, weight in enumerate(weights):
                        result = result + weight * value[:, p] * value[:, p]
                    tall = chunks * (height // len(weights))
                    power[pl.ds(pl.multiple_of(j * tall, 8), tall)] = result.reshape(tall, 128)
        return carry

    lax.fori_loop(0, pieces + lag, forward, 0)

    def drain(j, carry):
        for upward in (True, False):
            @pl.when(jnp.logical_not(ends(upward)))
            def _():
                hop(j, upward, inbox)[1].wait_send()
        return carry

    lax.fori_loop(0, pieces, drain, 0)

    near = groups * links // 2
    owner = jnp.logical_or(link == 0, link == links - 1)
    offset = jnp.where(low, 0, near)

    def deliver(index, target):
        at = pl.ds(pl.multiple_of(index * share, 8), share)
        return pltpu.make_async_remote_copy(
            src_ref=power.at[at],
            dst_ref=heard.at[my_class],
            send_sem=share_send.at[index],
            recv_sem=share_recv.at[my_class],
            device_id=member(target),
            device_id_type=MESH,
        )

    @pl.when(owner)
    def _():
        def send(index, carry):
            @pl.when(index + offset != me)
            def _():
                deliver(index, index + offset).start()
            return carry

        lax.fori_loop(0, near, send, 0)
        here = me - offset
        heard[my_class] = power[pl.ds(pl.multiple_of(here * share, 8), share)]

    for other in range(groups):
        @pl.when(jnp.logical_not(jnp.logical_and(owner, my_class == other)))
        def _():
            pltpu.make_async_remote_copy(
                src_ref=power.at[pl.ds(0, share)],
                dst_ref=heard.at[other],
                send_sem=share_send.at[0],
                recv_sem=share_recv.at[other],
                device_id=member(lax.rem(me + 1, family)),
                device_id_type=MESH,
            ).wait_recv()

    out[...] = jnp.sum(heard[...], axis=0)

    @pl.when(owner)
    def _():
        def finish(index, carry):
            @pl.when(index + offset != me)
            def _():
                deliver(index, index + offset).wait_send()
            return carry

        lax.fori_loop(0, near, finish, 0)


def chain(partial, chunks, collective_id):
    bands, grids = lax.axis_size("band"), lax.axis_size("grid")
    groups, links = bands // 2 * 2, grids // 2
    height = partial.shape[0] // chunks
    near = groups * links // 2
    kept = height // len(PAIRS)
    share = chunks // 2 // near * kept
    pieces = math.gcd(chunks // 2, 16)
    dma = pltpu.SemaphoreType.DMA
    return pl.pallas_call(
        functools.partial(chain_kernel, pieces, share, height, tuple(p[2] for p in PAIRS)),
        out_shape=jax.ShapeDtypeStruct((share, 128), F32),
        in_specs=[pl.BlockSpec(memory_space=pltpu.VMEM)],
        out_specs=pl.BlockSpec(memory_space=pltpu.VMEM),
        scratch_shapes=[
            pltpu.VMEM(partial.shape, F32),
            pltpu.VMEM((chunks // 2 * kept, 128), F32),
            pltpu.VMEM((groups, share, 128), F32),
            dma((pieces,)), dma((pieces,)), dma((pieces,)), dma((pieces,)),
            dma((near,)), dma((groups,)),
        ],
        compiler_params=pltpu.CompilerParams(
            collective_id=collective_id, has_side_effects=True, vmem_limit_bytes=VMEM_LIMIT
        ),
        name="chain",
    )(partial)


def sum_kernel(axis, count, mine, total, inbox, send_sem, recv_sem):
    me = lax.axis_index(axis)
    barrier = pltpu.get_barrier_semaphore()
    for p in range(1, count):
        peer = lax.rem(me + p, count)
        pl.semaphore_signal(barrier, inc=1, device_id={axis: peer}, device_id_type=MESH)
    pl.semaphore_wait(barrier, count - 1)
    copies = []
    for p in range(1, count):
        copy = pltpu.make_async_remote_copy(
            src_ref=mine,
            dst_ref=inbox.at[me],
            send_sem=send_sem.at[p - 1],
            recv_sem=recv_sem.at[p - 1],
            device_id={axis: lax.rem(me + p, count)},
            device_id_type=MESH,
        )
        copy.start()
        copies.append(copy)
    inbox[me] = mine[...]
    for copy in copies:
        copy.wait()
    total[...] = jnp.sum(inbox[...], axis=0)


def sum_over(block, axis, collective_id):
    count = lax.axis_size(axis)
    return pl.pallas_call(
        functools.partial(sum_kernel, axis, count),
        out_shape=jax.ShapeDtypeStruct(block.shape, block.dtype),
        in_specs=[pl.BlockSpec(memory_space=pltpu.VMEM)],
        out_specs=pl.BlockSpec(memory_space=pltpu.VMEM),
        scratch_shapes=[
            pltpu.VMEM((count,) + block.shape, block.dtype),
            pltpu.SemaphoreType.DMA((count - 1,)),
            pltpu.SemaphoreType.DMA((count - 1,)),
        ],
        compiler_params=pltpu.CompilerParams(collective_id=collective_id, has_side_effects=True),
    )(block)


def constant_tables(slab_x, grids, size_y, size_z):
    size_x = slab_x * grids
    half = slab_x // 2
    depth = -(-half // 8) * 8
    quarter = size_y // 4
    rows = -(-(quarter + 1) // 8) * 8
    cells = float(size_x) * size_y * size_z
    bases = []
    for core in range(2):
        cosine, sine = trig(quarter * core + np.arange(quarter + 1), np.arange(size_y), size_y)
        stack = np.zeros((2, rows, size_y))
        stack[0, : quarter + 1], stack[1, : quarter + 1] = cosine / cells, sine / cells
        bases.append(stack.reshape(2 * rows, size_y))
    high, low = halves(np.stack(bases))
    basis_wide = np.concatenate([high, high], axis=2)
    cosine, sine = trig(np.arange(size_z), np.arange(size_z), size_z)
    z_high, z_low = halves(np.concatenate([cosine, sine], axis=1))
    table_wide = np.concatenate([z_high, z_high], axis=0)
    odd = 2 * np.arange(depth) + 1
    cosine, sine = trig(odd, np.arange(size_x), 2 * size_x)
    turns = np.zeros((grids, 2 * depth + 8, size_x))
    turns[:, :depth], turns[:, depth : 2 * depth] = cosine, sine
    centre = 2 * slab_x * np.arange(grids) + slab_x - 1
    turns[:, 2 * depth], turns[:, 2 * depth + 1] = trig(centre, np.arange(size_x), 2 * size_x)
    return basis_wide, low, table_wide, z_low, turns.astype(np.float32)


def work_items(rows, slabs, slab_y):
    rows = rows.reshape(slabs, -1, 128)
    chunks = rows.shape[1]
    first, last = jnp.min(rows, axis=2), jnp.max(rows, axis=2)
    ends = jnp.cumsum(last - first + 1, axis=1)
    items = chunks + -(-slab_y // 4) * 4
    index = jnp.arange(items, dtype=jnp.int32)
    done = (ends[:, None, :] <= index[None, :, None]).astype(jnp.int32)
    chunk = jnp.minimum(jnp.sum(done, axis=2), chunks - 1)
    hot = (chunk[:, :, None] == jnp.arange(chunks, dtype=jnp.int32)).astype(jnp.int32)
    pick = lambda a: jnp.sum(hot * a[:, None, :], axis=2)
    row = pick(last) + 1 + index[None, :] - pick(ends)
    row = jnp.where(index[None, :] < ends[:, -1:], row, -1)
    return chunk.reshape(-1).astype(jnp.int32), row.reshape(-1).astype(jnp.int32)


def cosine_of_turns(turns):
    nodes = 0.25 * np.cos((np.arange(400) + 0.5) * np.pi / 400)
    powers = nodes[:, None] ** (2 * np.arange(6)[None, :])
    fit = np.linalg.lstsq(powers, np.sin(TWO_PI * nodes) / nodes, rcond=None)[0]
    u = 0.25 - jnp.abs(turns)
    square = u * u
    value = jnp.full_like(square, fit[5])
    for c in fit[4::-1]:
        value = value * square + np.float32(c)
    return u * value


def swap(value, pairs):
    return lax.ppermute(value, ("band", "grid"), pairs)


def per_device(orbitals, occupation, g_list, positions, species, widths):
    bands, slab_x, size_y, size_z = orbitals.shape
    grids, groups = lax.axis_size("grid"), lax.axis_size("band")
    assert bands == 2 and groups == 4 and grids % 4 == 0
    size_x = slab_x * grids
    slab_y = size_y // grids
    grid, band = lax.axis_index("grid"), lax.axis_index("band")
    core, x = band % 2, band // 2
    mate, link = grid % 2, grid // 2
    links = grids // 2

    plane = size_x * size_z
    line = slab_y * size_z
    key = g_list // size_z % slab_y * plane + g_list // line * size_z + g_list % size_z
    lists = lax.all_gather(lax.sort(key), "grid")

    own = orbitals * jnp.sqrt(occupation)[:, None, None, None]
    own, lists = lax.optimization_barrier((own, lists))

    every = [(b, g) for b in range(groups) for g in range(grids)]
    flat = lambda b, g: b * grids + g
    cross = lambda b: (b + 2) % 4
    to_mate = [(flat(b, g), flat(b, g ^ 1)) for b, g in every]
    to_core = [(flat(b, g), flat(b ^ 1, g)) for b, g in every]
    to_far = [(flat(b, g), flat(cross(b), g)) for b, g in every if b % 2 == g % 2]
    spread = [(flat(b, g), flat(b ^ 1, g)) for b, g in every if b % 2 == g % 2]
    other = swap(own, to_mate)
    leads = core == mate

    def whole_set(mine):
        beside = swap(mine, to_core)
        far = swap(mine, to_far)
        far = jnp.where(leads, far, swap(far, spread))
        return jnp.concatenate([mine, beside, far], axis=0)

    quarter = grids // 4
    order = np.concatenate([np.arange(quarter, grids), np.arange(quarter)]).reshape(2, grids // 2)
    lists = jnp.concatenate([lists[quarter:], lists[:quarter]], axis=0).reshape(2, -1)
    keys = jnp.where(core == 1, lists[0], lists[1])
    slabs = jnp.where(core == 1, order[0], order[1])
    y_of = jnp.repeat(slabs * slab_y, g_list.shape[0]) + keys // plane
    x_of = keys // size_z % size_x
    z_of = keys % size_z
    upper = jnp.repeat(slabs >= grids // 2, g_list.shape[0])
    row = jnp.where(upper, size_y - y_of, y_of) - core * (size_y // 4)
    x_fold = jnp.where(upper, (size_x - x_of) % size_x, x_of)
    z_fold = jnp.where(upper, (size_z - z_of) % size_z, z_of)
    chunks = keys.shape[0] // CHUNK
    shaped = [a.reshape(-1, 128) for a in (row, x_fold, z_fold)]
    entries = jnp.stack(shaped + [shaped[0]] * 5, axis=1).astype(jnp.int32)
    item_chunk, item_row = work_items(shaped[0], grids // 2, slab_y)

    share = chunks // (4 * links)
    place = (link % (links // 2)) * 4 + x * 2 + mate + jnp.where(link < links // 2, 0, chunks // share // 2)
    folded = lambda cell, size: jnp.where(cell < size // 2, cell, cell - size).astype(F32)
    mine = lambda a: lax.dynamic_slice(a, (place * share * CHUNK,), (share * CHUNK,))
    kx, ky, kz = (folded(mine(a), n) for a, n in ((x_of, size_x), (y_of, size_y), (z_of, size_z)))
    gx, gy, gz = TWO_PI / size_x * kx, TWO_PI / size_y * ky, TWO_PI / size_z * kz
    square = gx * gx + gy * gy + gz * gz
    nonzero = (square > 0).astype(F32)
    inverse = nonzero / (square + 1.0 - nonzero)
    coulomb = 4.0 * math.pi * inverse
    turns = (
        kx[:, None] * positions[0][None, :]
        + ky[:, None] * positions[1][None, :]
        + kz[:, None] * positions[2][None, :]
    )
    turns = turns - jnp.round(turns)
    width = widths[species]
    waves = jnp.exp(-0.5 * square[:, None] * (width * width)[None, :]) * cosine_of_turns(turns)

    tables = constant_tables(slab_x, grids, size_y, size_z)
    pick = lambda table, index: lax.dynamic_index_in_dim(jnp.asarray(table), index, 0, keepdims=False)
    held = (pick(tables[0], core), pick(tables[1], core), jnp.asarray(tables[2]), jnp.asarray(tables[3]))
    main = jnp.where(core == (x + mate) % 2, 0, 1)
    band_of = [2 * main, 2 * main + 1, 2 - 2 * main + mate, 2 - 2 * main + 1 - mate, 4, 5]
    chosen = jnp.stack(
        [jnp.stack([jnp.asarray(band_of[i], jnp.int32) for i in pair[:2]]) for pair in PAIRS]
    )

    partial = select(
        chosen, item_chunk, item_row, whole_set(own), entries, grids // 2, held, pick(tables[4], grid), None
    )
    partial, far_set, waves = lax.optimization_barrier((partial, whole_set(other), waves))
    partial = select(
        chosen, item_chunk, item_row, far_set, entries, grids // 2, held,
        pick(tables[4], grid + 1 - 2 * mate), partial,
    )
    power = chain(partial, chunks, 0)
    tiles = CHUNK // 128
    power = power.reshape(share, 2, tiles, 128)
    weighted = (power[:, 0] + power[:, 1]).reshape(-1) * coulomb
    reduced = 2.0 * weighted * inverse
    total = jnp.sum(weighted)
    xx = jnp.sum(reduced * gx * gx) - total
    yy = jnp.sum(reduced * gy * gy) - total
    zz = jnp.sum(reduced * gz * gz) - total
    xy = jnp.sum(reduced * gx * gy)
    xz = jnp.sum(reduced * gx * gz)
    yz = jnp.sum(reduced * gy * gz)
    stress = jnp.stack([xx, xy, xz, xy, yy, yz, xz, yz, zz])
    atoms = jnp.dot(weighted[None, :], waves, precision=HIGHEST)[0]
    out = jnp.concatenate([stress, atoms]) / float(bands * groups)
    size = out.shape[0]
    padded = -(-size // 1024) * 1024
    block = jnp.pad(out, (0, padded - size)).reshape(padded // 128, 128)
    out = sum_over(sum_over(block, "grid", 1), "band", 2).reshape(-1)[:size]
    return out[:9].reshape(3, 3), out[9:]


def solution(mesh):
    return jax.shard_map(
        per_device,
        mesh=mesh,
        in_specs=(P("band", "grid", None, None), P("band"), P("grid"), P(), P(), P()),
        out_specs=(P(), P()),
        check_vma=False,
    )
```

```python
import functools
import math

import jax
import jax.numpy as jnp
import numpy as np
from jax import lax
from jax.experimental import pallas as pl
from jax.experimental.pallas import tpu as pltpu
from jax.sharding import PartitionSpec as P

HIGHEST = lax.Precision.HIGHEST
MESH = pl.DeviceIdType.MESH
TWO_PI = 2.0 * math.pi
F32 = jnp.float32
BF16 = jnp.bfloat16
LANES = 128
DEPTH = 8
HOP_LAG = 4
CUTS = 4
VMEM_LIMIT = 63 * 1024 * 1024

BATCHES = (
    ((0, 0, 1.0), (0, 1, 2.0), (1, 1, 1.0), (0, 2, 2.0), (1, 3, 2.0)),
    ((0, 4, 2.0), (0, 5, 2.0), (1, 4, 2.0), (1, 5, 2.0)),
)


def trig(rows, columns, length):
    angles = TWO_PI / length * (rows[:, None] * columns[None, :] % length)
    return np.cos(angles), np.sin(angles)


def halves(table):
    table = np.asarray(table, np.float32)
    high = table.astype(jnp.bfloat16)
    low = (table - high.astype(np.float32)).astype(jnp.bfloat16)
    return high, low


def split(value):
    high = value.astype(BF16)
    low = (value - high.astype(F32)).astype(BF16)
    return high, low


def dot(a, b):
    return jnp.dot(a, b, preferred_element_type=F32)


def constant_tables(slab_x, grids, size_y, size_z):
    size_x = slab_x * grids
    half = slab_x // 2
    depth = DEPTH
    assert half <= depth
    quarter = size_y // 4
    rows = -(-(quarter + 1) // 8) * 8
    cells = float(size_x) * size_y * size_z
    bases = []
    for core in range(2):
        cosine, sine = trig(quarter * core + np.arange(quarter + 1), np.arange(size_y), size_y)
        stack = np.zeros((2, rows, size_y))
        stack[0, : quarter + 1], stack[1, : quarter + 1] = cosine / cells, sine / cells
        bases.append(stack.reshape(2 * rows, size_y))
    high, low = halves(np.stack(bases))
    basis_wide = np.concatenate([high, high], axis=2)
    cosine, sine = trig(np.arange(size_z), np.arange(size_z), size_z)
    z_high, z_low = halves(np.concatenate([cosine, sine], axis=1))
    table_wide = np.concatenate([z_high, z_high], axis=0)
    odd = 2 * np.arange(depth) + 1
    cosine, sine = trig(odd, np.arange(size_x), 2 * size_x)
    turns = np.zeros((grids, 2 * depth + 8, size_x))
    turns[:, :depth], turns[:, depth : 2 * depth] = cosine, sine
    centre = 2 * slab_x * np.arange(grids) + slab_x - 1
    turns[:, 2 * depth], turns[:, 2 * depth + 1] = trig(centre, np.arange(size_x), 2 * size_x)
    return basis_wide, low, table_wide, z_low, turns.astype(np.float32)


def cosine_of_turns(turns):
    nodes = 0.25 * np.cos((np.arange(400) + 0.5) * np.pi / 400)
    powers = nodes[:, None] ** (2 * np.arange(6)[None, :])
    fit = np.linalg.lstsq(powers, np.sin(TWO_PI * nodes) / nodes, rcond=None)[0]
    u = 0.25 - jnp.abs(turns)
    square = u * u
    value = jnp.full_like(square, float(fit[5]))
    for c in fit[4::-1]:
        value = value * square + float(c)
    return u * value


def pad_kernel(planes, items, ends, at, codes, out):
    out[...] = jnp.full_like(out, -1)
    lane = lax.broadcasted_iota(jnp.int32, (1, LANES), 1)
    flat = lax.broadcasted_iota(jnp.int32, (8, LANES), 0) * LANES + lax.broadcasted_iota(jnp.int32, (8, LANES), 1)

    def one_plane(k, carry):
        start = jnp.where(k == 0, 0, ends[jnp.maximum(k - 1, 0)])
        end = ends[k]
        count = lax.div(end - start + LANES - 1, LANES)

        def one_row(c, carry):
            place, marks = carry
            source = start + c * LANES
            row, shift = lax.div(source, LANES), lax.rem(source, LANES)
            index = jnp.broadcast_to(lax.rem(lane + shift, LANES), (8, LANES))
            pick = lambda r: jnp.take_along_axis(
                jnp.broadcast_to(codes[pl.ds(r, 1), :], (8, LANES)), index, axis=1
            )[0:1]
            value = jnp.where(lane + shift < LANES, pick(row), pick(row + 1))
            out[pl.ds(place, 1), :] = jnp.where(source + lane < end, value, -1)
            return place + 1, jnp.where(flat == place, at[0] + at[1] * k, marks)

        return lax.fori_loop(0, count, one_row, carry)

    marks = lax.fori_loop(0, planes, one_plane, (0, jnp.zeros((8, LANES), jnp.int32)))[1]
    out[pl.ds(items, 8), :] = marks


def pad_planes(codes, ends, at, items):
    return pl.pallas_call(
        functools.partial(pad_kernel, ends.shape[0], items),
        out_shape=jax.ShapeDtypeStruct((items + 8, LANES), jnp.int32),
        grid_spec=pltpu.PrefetchScalarGridSpec(
            num_scalar_prefetch=2,
            grid=(1,),
            in_specs=[pl.BlockSpec(codes.shape, lambda i, *_: (0, 0))],
            out_specs=pl.BlockSpec((items + 8, LANES), lambda i, *_: (0, 0)),
        ),
        name="pad_planes",
    )(ends, at, codes)


def exchange_kernel(
    plan,
    own, listing, atoms, basis_wide, basis_low, table_wide, table_low, turns, out,
    store, planes_a, planes_b, part_a, part_b, box_a, box_b, lists, marks, power, heard, votes, waves, sums,
    list_send, list_recv, mark_sem, side_send, side_recv, mate_send, mate_recv, lane_send, lane_recv,
    far_send, far_recv, hand_send, hand_recv, away_send, away_recv, pass_send, pass_recv, copy_sem,
    hop_send, hop_recv, share_send, share_recv, vote_send, vote_recv,
):
    size_x, slabs, items, pieces, share, kept = plan
    band, grid = lax.axis_index("band"), lax.axis_index("grid")
    bands, grids = lax.axis_size("band"), lax.axis_size("grid")
    core, x = lax.rem(band, 2), lax.div(band, 2)
    mate, link = lax.rem(grid, 2), lax.div(grid, 2)
    links = grids // 2
    everyone = bands * grids
    me = band * grids + grid
    slab_x, size_y, size_z = own.shape[1:]
    planes, parts, boxes = (planes_a, planes_b), (part_a, part_b), (box_a, box_b)
    leads = core == mate
    quarter = grids // 4
    height = items + 8
    rows = basis_low.shape[0] // 2
    kept_rows = size_y // 4 + 1

    def at(index):
        return {"band": lax.div(index, grids), "grid": lax.rem(index, grids)}

    barrier = pltpu.get_barrier_semaphore()

    def greet(step, carry):
        pl.semaphore_signal(barrier, inc=1, device_id=at(lax.rem(me + step, everyone)), device_id_type=MESH)
        return carry

    lax.fori_loop(1, everyone, greet, 0)
    pl.semaphore_wait(barrier, everyone - 1)

    def remote(source, target, send, recv, device):
        return pltpu.make_async_remote_copy(
            src_ref=source, dst_ref=target, send_sem=send, recv_sem=recv,
            device_id=device, device_id_type=MESH,
        )

    beside = {"band": band + 1 - 2 * core}
    across = {"grid": grid + 1 - 2 * mate}
    far = {"band": lax.rem(band + bands // 2, bands)}

    slot_of = lambda g, c: lax.rem(g + grids - jnp.where(c == 1, quarter, 3 * quarter), grids)
    middle = jnp.logical_and(grid >= quarter, grid < 3 * quarter)
    lists_here = middle == (core == 1)
    my_slot = slot_of(grid, core)

    def list_copy(slot, step):
        return remote(
            listing, lists.at[pl.ds(pl.multiple_of(slot * height, 8), height)],
            list_send.at[step - 1], list_recv.at[slot], {"grid": lax.rem(grid + step, grids)},
        )

    own_list = pltpu.make_async_copy(
        listing, lists.at[pl.ds(pl.multiple_of(my_slot * height, 8), height)], copy_sem.at[1]
    )

    @pl.when(lists_here)
    def _():
        def send(step, carry):
            list_copy(my_slot, step).start()
            return carry

        lax.fori_loop(1, grids, send, 0)
        own_list.start()

    cut = slab_x // (CUTS // 2)
    place = lambda group, slab, c: store.at[(group * 2 + slab) * 2 + c % 2, pl.ds(c // 2 * cut, cut)]
    mine = lambda c: own.at[c % 2, pl.ds(c // 2 * cut, cut)]
    to_side = lambda c: remote(mine(c), place(1, 0, c), side_send.at[c], side_recv.at[c], beside)
    to_mate = lambda c: remote(mine(c), place(0, 1, c), mate_send.at[c], mate_recv.at[c], across)
    to_far = lambda c: remote(mine(c), place(2, 0, c), far_send.at[c], far_recv.at[c], far)
    hand_on = lambda c: remote(place(2, 0, c), place(2, 0, c), hand_send.at[c], hand_recv.at[c], beside)
    mate_side = lambda c: remote(place(0, 1, c), place(1, 1, c), lane_send.at[c], lane_recv.at[c], beside)
    mate_far = lambda c: remote(place(0, 1, c), place(2, 1, c), away_send.at[c], away_recv.at[c], far)
    mate_hand = lambda c: remote(place(2, 1, c), place(2, 1, c), pass_send.at[c], pass_recv.at[c], beside)
    keep = pltpu.make_async_copy(own, store.at[pl.ds(0, 2)], copy_sem.at[0])
    keep.start()
    for c in range(CUTS):
        to_side(c).start()
        to_mate(c).start()

    @pl.when(leads)
    def _():
        for c in range(CUTS):
            to_far(c).start()

    def relay_far(c):
        @pl.when(leads)
        def _():
            to_far(c).wait_recv()
            hand_on(c).start()

    def relay_mate(c):
        to_mate(c).wait_recv()
        mate_side(c).start()

        @pl.when(leads)
        def _():
            mate_far(c).start()

    def relay_mate_far(c):
        @pl.when(leads)
        def _():
            mate_far(c).wait_recv()
            mate_hand(c).start()

    main = jnp.where(core == lax.rem(x + mate, 2), 0, 1)
    other = 1 - main
    base_of = (
        main * 4, main * 4 + 1, other * 4 + mate, other * 4 + 1 - mate, 8, 9,
    )

    def transform(batch, slab):
        pairs, target = BATCHES[batch], planes[batch]
        width = len(pairs) * 4 * DEPTH
        half = slab_x // 2
        unroll = math.gcd(half, 4)
        pick = lambda which, p: sum(
            jnp.where(p == q, base_of[pair[which]], 0) for q, pair in enumerate(pairs)
        ) + 2 * slab
        if half < DEPTH and slab == 0:
            target[...] = jnp.zeros_like(target)

        flat = target.reshape(kept_rows * width, size_z)

        def one_pair(p, carry):
            left, right = pick(0, p), pick(1, p)
            for block in range(half // unroll):
                stack = []
                for u in range(unroll):
                    up = half + block * unroll + u
                    down = half - 1 - block * unroll - u
                    above = store[left, up] * store[right, up]
                    below = store[left, down] * store[right, down]
                    stack += [above + below, above - below]
                high, low = split(jnp.concatenate(stack, axis=1))
                along = dot(basis_wide[...], jnp.concatenate([high, low], axis=0))
                along = along + dot(basis_low[...], high)
                stack = [along[:, i * size_z : (i + 1) * size_z] for i in range(2 * unroll)]
                high, low = split(jnp.concatenate(stack, axis=0))
                both = dot(jnp.concatenate([high, low], axis=1), table_wide[...])
                both = both + dot(high, table_low[...])
                for u in range(unroll):
                    for sign in range(2):
                        begin = (2 * u + sign) * 2 * rows
                        cosine, sine = both[begin : begin + rows], both[begin + rows : begin + 2 * rows]
                        real = cosine[:, :size_z] - sine[:, size_z:]
                        imag = -(cosine[:, size_z:] + sine[:, :size_z])
                        for part, value in ((0, real), (1, imag)):
                            row = (p * 4 + 2 * sign + part) * DEPTH + block * unroll + u
                            flat[pl.ds(row, kept_rows, stride=width), :] = value[:kept_rows]
            return carry

        lax.fori_loop(0, len(pairs), one_pair, 0)

    def code_row(t):
        slot, r = lax.div(t, items), lax.rem(t, items)
        return slot, r, lists[pl.ds(slot * height + r, 1), :]

    def select(batch, slab, group):
        pairs, source, part = BATCHES[batch], planes[batch], parts[batch]
        count = len(pairs)
        for u in range(4):
            slot, r, code = code_row(group * 4 + u)
            k = marks[slot * 8 + lax.div(r, LANES), lax.rem(r, LANES)]
            x_of = jnp.broadcast_to(lax.shift_right_arithmetic(code, size_z.bit_length() - 1) & (size_x - 1), (8, LANES))
            z_of = jnp.broadcast_to(code & (size_z - 1), (8, LANES))
            turn = lambda i: jnp.take_along_axis(turns[slab, pl.ds(8 * i, 8), :], x_of, axis=1)
            cosine, sine, phase = turn(0), turn(1), turn(2)
            phase_cos, phase_sin = phase[0:1], phase[1:2]
            for p in range(count):
                get = lambda i: jnp.take_along_axis(source[k, pl.ds((p * 4 + i) * 8, 8), :], z_of, axis=1)
                real = jnp.sum(get(0) * cosine + get(3) * sine, axis=0, keepdims=True)
                imag = jnp.sum(get(1) * cosine - get(2) * sine, axis=0, keepdims=True)
                for which, value in (
                    (0, real * phase_cos + imag * phase_sin),
                    (4, imag * phase_cos - real * phase_sin),
                ):
                    row = pl.ds(group * (8 * count) + p * 8 + which + u, 1)
                    part[row, :] = value if slab == 0 else part[row, :] + value

    groups = slabs * items // 4
    half_groups = groups // 2
    piece = half_groups // pieces

    begins = lambda upward: link == (0 if upward else links - 1)
    ends = lambda upward: link == (links - 1 if upward else 0)

    def hop(batch, upward, j, source):
        tall = piece * 8 * len(BATCHES[batch])
        rows_at = pl.ds(pl.multiple_of((j + (pieces if upward else 0)) * tall, 8), tall)
        sem = ((batch * 2 + (0 if upward else 1)) * pieces) + j
        step = 2 if upward else grids - 2
        return rows_at, remote(
            source.at[rows_at], boxes[batch].at[rows_at], hop_send.at[sem], hop_recv.at[sem],
            {"grid": lax.rem(grid + step, grids)},
        )

    def forward(batch, upward, j):
        at_rows, copy = hop(batch, upward, j, boxes[batch])
        copy.wait_recv()
        box, part = boxes[batch], parts[batch]
        box[at_rows] = box[at_rows] + part[at_rows]

        @pl.when(jnp.logical_not(ends(upward)))
        def _():
            copy.start()

        @pl.when(ends(upward))
        def _():
            value = box[at_rows].reshape(piece, len(BATCHES[batch]), 8, LANES)
            total = 0.0
            for p, pair in enumerate(BATCHES[batch]):
                total = total + pair[2] * value[:, p] * value[:, p]
            total = total.reshape(piece * 8, LANES)
            spot = pl.ds(pl.multiple_of(j * (piece * 8), 8), piece * 8)
            power[spot] = total if batch == 0 else power[spot] + total

    def chain_step(step):
        for upward in (True, False):
            hops = link if upward else links - 1 - link
            j = step - HOP_LAG * hops
            for batch in range(2):
                inside = jnp.logical_and(j >= batch * pieces, j < (batch + 1) * pieces)

                @pl.when(jnp.logical_and(inside, hops > 0))
                def _():
                    forward(batch, upward, j - batch * pieces)

    def wave_parts(t):
        slot, r, code = code_row(t)
        k = marks[slot * 8 + lax.div(r, LANES), lax.rem(r, LANES)]
        valid = code >= 0
        x_of = lax.shift_right_arithmetic(code, size_z.bit_length() - 1) & (size_x - 1)
        z_of = code & (size_z - 1)
        upper = jnp.where((slot >= quarter) == (core == 1), 1, 0)
        fold = lambda cell, size: jnp.where(cell < size // 2 + upper, cell, cell - size).astype(F32)
        kx, kz = fold(x_of, size_x), fold(z_of, size_z)
        ky = jnp.broadcast_to(k + core * (size_y // 4), (1, LANES)).astype(F32)
        gx, gy, gz = TWO_PI / size_x * kx, TWO_PI / size_y * ky, TWO_PI / size_z * kz
        square = gx * gx + gy * gy + gz * gz
        nonzero = jnp.where(square > 0, 1.0, 0.0)
        inverse = nonzero / (square + 1.0 - nonzero)
        inverse = jnp.where(valid, inverse, 0.0)
        return kx, ky, kz, gx, gy, gz, square, inverse

    count_atoms = atoms.shape[1]
    stride = 64

    def wave_block(values, b):
        kx, ky, kz = values[:3]
        at_atoms = pl.ds(b * stride, stride)
        turn = kx * atoms[0, at_atoms] + ky * atoms[1, at_atoms] + kz * atoms[2, at_atoms]
        turn = turn - jnp.floor(turn + 0.5)
        return jnp.exp(values[6] * atoms[3, at_atoms]) * cosine_of_turns(turn)

    near = 2 * (bands // 2) * links // 2
    my_class = x * 2 + mate
    offset = jnp.where(link < links // 2, 0, near)
    order = link * (2 * (bands // 2)) + my_class
    first_chunk = order * share

    for c in range(CUTS):
        to_side(c).wait_recv()
    keep.wait()
    transform(0, 0)

    for slot in range(slabs):
        from_here = jnp.logical_and(lists_here, my_slot == slot)

        @pl.when(jnp.logical_not(from_here))
        def _():
            list_copy(slot, 1).wait_recv()

        @pl.when(from_here)
        def _():
            own_list.wait()

    def mark_copy(slot):
        return pltpu.make_async_copy(
            lists.at[pl.ds(pl.multiple_of(slot * height + items, 8), 8)],
            marks.at[pl.ds(pl.multiple_of(slot * 8, 8), 8)], mark_sem.at[slot],
        )

    for slot in range(slabs):
        mark_copy(slot).start()
    for slot in range(slabs):
        mark_copy(slot).wait()

    def select_run(batch, slab, low, high):
        def body(group, carry):
            select(batch, slab, group)
            return carry

        lax.fori_loop(low, high, body, 0)

    spans = [groups * i // CUTS for i in range(CUTS + 1)]
    for c in range(CUTS):
        relay_far(c)
        select_run(0, 0, spans[c], spans[c + 1])
        if c < CUTS // 2:
            relay_mate(c)

    @pl.when(jnp.logical_not(leads))
    def _():
        for c in range(CUTS):
            hand_on(c).wait_recv()

    transform(1, 0)
    for c in range(CUTS):
        if c < CUTS // 2:
            relay_mate(c + CUTS // 2)
        relay_mate_far(c)
        select_run(1, 0, spans[c], spans[c + 1])

    for c in range(CUTS):
        mate_side(c).wait_recv()
    transform(0, 1)

    def one_piece(batch):
        def body(i, carry):
            for upward in (True, False):
                base = (i + (pieces if upward else 0)) * piece
                select_run(batch, 1, base, base + piece)

                @pl.when(begins(upward))
                def _():
                    hop(batch, upward, i, parts[batch])[1].start()

            chain_step(i + batch * pieces)
            return carry

        return body

    lax.fori_loop(0, pieces, one_piece(0), 0)

    @pl.when(jnp.logical_not(leads))
    def _():
        for c in range(CUTS):
            mate_hand(c).wait_recv()

    transform(1, 1)
    lax.fori_loop(0, pieces, one_piece(1), 0)

    def keep_wave(q, carry):
        values = wave_parts(first_chunk + q)
        for b in range(count_atoms // stride):
            waves[q, pl.ds(b * stride, stride)] = wave_block(values, b)
        return carry

    def run_out(step, carry):
        chain_step(step)
        return carry

    last = 2 * pieces
    lax.fori_loop(0, kept, keep_wave, 0)
    lax.fori_loop(last, last + HOP_LAG * (links - 1), run_out, 0)

    owner = jnp.logical_or(link == 0, link == links - 1)

    def member(index):
        at_link, at_class = lax.div(index, 2 * (bands // 2)), lax.rem(index, 2 * (bands // 2))
        return {"band": lax.div(at_class, 2) * 2 + core, "grid": at_link * 2 + lax.rem(at_class, 2)}

    tall = share * 2

    def deliver(index):
        return remote(
            power.at[pl.ds(pl.multiple_of(index * tall, 8), tall)], heard.at[my_class],
            share_send.at[index], share_recv.at[my_class], member(index + offset),
        )

    @pl.when(owner)
    def _():
        def send(index, carry):
            @pl.when(index + offset != order)
            def _():
                deliver(index).start()
            return carry

        lax.fori_loop(0, near, send, 0)
        heard[my_class] = power[pl.ds(pl.multiple_of((order - offset) * tall, 8), tall)]

    for sender in range(2 * (bands // 2)):
        @pl.when(jnp.logical_not(jnp.logical_and(owner, my_class == sender)))
        def _():
            remote(
                power.at[pl.ds(0, tall)], heard.at[sender], share_send.at[0], share_recv.at[sender],
                {"grid": lax.rem(grid + 2, grids)},
            ).wait_recv()

    total = heard[0]
    for sender in range(1, 2 * (bands // 2)):
        total = total + heard[sender]
    heard[0] = total

    zero = jnp.zeros((1, LANES), F32)

    def weigh(stored):
        def body(q, carry):
            sums, stress = carry
            values = wave_parts(first_chunk + q)
            gx, gy, gz, inverse = values[3], values[4], values[5], values[7]
            row = lax.div(q, 4) * 8 + lax.rem(q, 4)
            selected = heard[0, pl.ds(row, 1), :] + heard[0, pl.ds(row + 4, 1), :]
            weighted = selected * (4.0 * math.pi) * inverse
            reduced = 2.0 * weighted * inverse
            terms = (
                weighted, reduced * gx * gx, reduced * gy * gy, reduced * gz * gz,
                reduced * gx * gy, reduced * gx * gz, reduced * gy * gz,
            )
            stress = tuple(a + b for a, b in zip(stress, terms))
            for b in range(count_atoms // stride):
                where = pl.ds(b * stride, stride)
                wave = waves[q, where] if stored else wave_block(values, b)
                sums[where] = sums[where] + weighted * wave
            return sums, stress

        return body

    def weigh_all(stored, low, high, stress, sums):
        def body(q, stress):
            return weigh(stored)(q, (sums, stress))[1]

        return lax.fori_loop(low, high, body, stress)

    sums[...] = jnp.zeros((count_atoms, LANES), F32)
    stress = weigh_all(True, 0, kept, (zero,) * 7, sums)
    if kept < share:
        stress = weigh_all(False, kept, share, stress, sums)
    blocks = []
    for b in range(count_atoms // LANES):
        blocks.append(jnp.sum(sums[pl.ds(b * LANES, LANES)].T, axis=0, keepdims=True))
    ballot = jnp.concatenate(blocks + list(stress), axis=0)
    out[...] = jnp.zeros_like(out)
    out[pl.ds(0, ballot.shape[0])] = ballot

    def vote(step):
        return remote(
            out, votes.at[me], vote_send.at[step - 1], vote_recv.at[step - 1],
            at(lax.rem(me + step, everyone)),
        )

    def cast(step, carry):
        vote(step).start()
        return carry

    def count_votes(step, carry):
        vote(step).wait_recv()
        return carry

    def settle(step, carry):
        vote(step).wait_send()
        return carry

    lax.fori_loop(1, everyone, cast, 0)
    votes[me] = out[...]

    for c in range(CUTS):
        to_side(c).wait_send()
        to_mate(c).wait_send()
        mate_side(c).wait_send()

        @pl.when(leads)
        def _():
            to_far(c).wait_send()
            hand_on(c).wait_send()
            mate_far(c).wait_send()
            mate_hand(c).wait_send()

    @pl.when(lists_here)
    def _():
        def sent(step, carry):
            list_copy(my_slot, step).wait_send()
            return carry

        lax.fori_loop(1, grids, sent, 0)

    for batch in range(2):
        def drain(j, carry):
            for upward in (True, False):
                @pl.when(jnp.logical_not(ends(upward)))
                def _():
                    hop(batch, upward, j, boxes[batch])[1].wait_send()
            return carry

        lax.fori_loop(0, pieces, drain, 0)

    @pl.when(owner)
    def _():
        def finish(index, carry):
            @pl.when(index + offset != order)
            def _():
                deliver(index).wait_send()
            return carry

        lax.fori_loop(0, near, finish, 0)

    lax.fori_loop(1, everyone, count_votes, 0)
    lax.fori_loop(1, everyone, settle, 0)
    result = votes[0]
    result = lax.fori_loop(1, everyone, lambda i, total: total + votes[i], result)
    out[...] = result


def exchange(own, listing, atoms, tables, turns, size_x, slabs, items):
    bands, grids = lax.axis_size("band"), lax.axis_size("grid")
    links, everyone = grids // 2, bands * grids
    pair, slab_x, size_y, size_z = own.shape
    groups = slabs * items // 4
    pieces = math.gcd(groups // 2, 12)
    near = 2 * (bands // 2) * links // 2
    share = slabs * items // 2 // near
    assert share % 4 == 0 and groups % 2 == 0
    counts = [len(b) for b in BATCHES]
    kept_rows = size_y // 4 + 1
    count_atoms = atoms.shape[1]
    mib = 1024 * 1024
    used = 4 * LANES * (
        6 * pair * slab_x * size_y + kept_rows * sum(counts) * 4 * DEPTH + 2 * groups * 8 * sum(counts)
        + slabs * (items + 8) + groups * 4 + 4 * share * 2 + everyone * 16
        + pair * slab_x * size_y + 4 * count_atoms + 4000
    )
    kept = max(0, min(share, (VMEM_LIMIT - 3 * mib - used) // (4 * LANES * count_atoms)))
    plan = (size_x, slabs, items, pieces, share, kept)
    vmem = pl.BlockSpec(memory_space=pltpu.VMEM)
    dma = lambda n: pltpu.SemaphoreType.DMA((n,))
    cut = lambda: dma(CUTS)
    ins = [own, listing, atoms, *tables, turns]
    return pl.pallas_call(
        functools.partial(exchange_kernel, plan),
        out_shape=jax.ShapeDtypeStruct((16, LANES), F32),
        in_specs=[vmem] * len(ins),
        out_specs=vmem,
        scratch_shapes=[
            pltpu.VMEM((6 * pair, slab_x, size_y, size_z), F32),
            *[pltpu.VMEM((kept_rows, n * 4 * DEPTH, size_z), F32) for n in counts],
            *[pltpu.VMEM((groups * 8 * n, LANES), F32) for n in counts],
            *[pltpu.VMEM((groups * 8 * n, LANES), F32) for n in counts],
            pltpu.VMEM((slabs * (items + 8), LANES), jnp.int32),
            pltpu.SMEM((slabs * 8, LANES), jnp.int32),
            pltpu.VMEM((groups // 2 * 8, LANES), F32),
            pltpu.VMEM((2 * (bands // 2), share * 2, LANES), F32),
            pltpu.VMEM((everyone, 16, LANES), F32),
            pltpu.VMEM((max(kept, 1), count_atoms, LANES), F32),
            pltpu.VMEM((count_atoms, LANES), F32),
            dma(grids - 1), dma(slabs), dma(slabs),
            cut(), cut(), cut(), cut(), cut(), cut(), cut(), cut(),
            cut(), cut(), cut(), cut(), cut(), cut(), dma(2),
            dma(4 * pieces), dma(4 * pieces),
            dma(near), dma(2 * (bands // 2)),
            dma(everyone - 1), dma(everyone - 1),
        ],
        compiler_params=pltpu.CompilerParams(
            collective_id=0, has_side_effects=True, vmem_limit_bytes=VMEM_LIMIT
        ),
        name="exchange",
    )(*ins)


def per_device(orbitals, occupation, g_list, positions, species, widths):
    bands, slab_x, size_y, size_z = orbitals.shape
    grids, groups = lax.axis_size("grid"), lax.axis_size("band")
    size_x = slab_x * grids
    slab_y = size_y // grids
    assert bands == 2 and groups == 4 and grids % 4 == 0 and size_z == LANES and size_x == LANES
    grid, band = lax.axis_index("grid"), lax.axis_index("band")
    core, mate = band % 2, grid % 2

    plane = size_x * size_z
    key = g_list // size_z % slab_y * plane + g_list // (slab_y * size_z) * size_z + g_list % size_z
    key = lax.sort(key)
    upper = grid >= grids // 2
    x_of, z_of = key // size_z % size_x, key % size_z
    x_of = jnp.where(upper, (size_x - x_of) % size_x, x_of)
    z_of = jnp.where(upper, (size_z - z_of) % size_z, z_of)
    codes = (x_of * size_z + z_of).astype(jnp.int32).reshape(-1, LANES)
    codes = jnp.pad(codes, ((0, 8), (0, 0)))
    ends = jnp.sum((key[None, :] < (jnp.arange(slab_y)[:, None] + 1) * plane).astype(jnp.int32), axis=1)
    middle = ((grid >= grids // 4) & (grid < 3 * grids // 4)).astype(jnp.int32)
    first = jnp.where(upper, size_y - grid * slab_y, grid * slab_y) - middle * (size_y // 4)
    at = jnp.stack([first, jnp.where(upper, -1, 1)]).astype(jnp.int32)
    items = g_list.shape[0] // LANES + -(-slab_y // 16) * 16
    listing = pad_planes(codes, ends.astype(jnp.int32), at, items)

    own = orbitals * jnp.sqrt(occupation)[:, None, None, None]
    width = widths[species]
    atoms = jnp.concatenate([positions, (-0.5 * width * width)[None, :]], axis=0)
    atoms = jnp.broadcast_to(atoms[:, :, None], atoms.shape + (LANES,))
    tables = constant_tables(slab_x, grids, size_y, size_z)
    pick = lambda table, index: lax.dynamic_index_in_dim(jnp.asarray(table), index, 0, keepdims=False)
    held = (pick(tables[0], core), pick(tables[1], core), jnp.asarray(tables[2]), jnp.asarray(tables[3]))
    turns = jnp.stack([pick(tables[4], grid), pick(tables[4], grid + 1 - 2 * mate)])

    out = exchange(own, listing, atoms, held, turns, size_x, grids // 2, items) / float(bands * groups)
    count = positions.shape[1]
    rows = count // LANES
    total, xx, yy, zz, xy, xz, yz = [jnp.sum(out[rows + i]) for i in range(7)]
    stress = jnp.stack([xx - total, xy, xz, xy, yy - total, yz, xz, yz, zz - total]).reshape(3, 3)
    return stress, out[:rows].reshape(-1)


def solution(mesh):
    return jax.shard_map(
        per_device,
        mesh=mesh,
        in_specs=(P("band", "grid", None, None), P("band"), P("grid"), P(), P(), P()),
        out_specs=(P(), P()),
        check_vma=False,
    )
```

```python
import functools
import math

import jax
import jax.numpy as jnp
import numpy as np
from jax import lax
from jax.experimental import pallas as pl
from jax.experimental.pallas import tpu as pltpu
from jax.sharding import PartitionSpec as P

HIGHEST = lax.Precision.HIGHEST
MESH = pl.DeviceIdType.MESH
TWO_PI = 2.0 * math.pi
F32 = jnp.float32
BF16 = jnp.bfloat16
LANES = 128
DEPTH = 8
RUN = 3
HOP_LAG = 4
CUTS = 4
VMEM_LIMIT = 63 * 1024 * 1024

BATCHES = (
    ((0, 0, 1.0), (0, 1, 2.0), (1, 1, 1.0), (0, 2, 2.0), (1, 3, 2.0)),
    ((0, 4, 2.0), (0, 5, 2.0), (1, 4, 2.0), (1, 5, 2.0)),
)


def trig(rows, columns, length):
    angles = TWO_PI / length * (rows[:, None] * columns[None, :] % length)
    return np.cos(angles), np.sin(angles)


def halves(table):
    table = np.asarray(table, np.float32)
    high = table.astype(jnp.bfloat16)
    low = (table - high.astype(np.float32)).astype(jnp.bfloat16)
    return high, low


def split(value):
    high = value.astype(BF16)
    low = (value - high.astype(F32)).astype(BF16)
    return high, low


def dot(a, b):
    return jnp.dot(a, b, preferred_element_type=F32)


def constant_tables(slab_x, grids, size_y, size_z):
    size_x = slab_x * grids
    half = slab_x // 2
    depth = DEPTH
    assert half <= depth
    quarter = size_y // 4
    rows = -(-(quarter + 1) // 8) * 8
    cells = float(size_x) * size_y * size_z
    bases = []
    for core in range(2):
        cosine, sine = trig(quarter * core + np.arange(quarter + 1), np.arange(size_y), size_y)
        stack = np.zeros((2, rows, size_y))
        stack[0, : quarter + 1], stack[1, : quarter + 1] = cosine / cells, sine / cells
        bases.append(stack.reshape(2 * rows, size_y))
    high, low = halves(np.stack(bases))
    basis_wide = np.concatenate([high, high], axis=2)
    cosine, sine = trig(np.arange(size_z), np.arange(size_z), size_z)
    z_high, z_low = halves(np.concatenate([cosine, sine], axis=1))
    table_wide = np.concatenate([z_high, z_high], axis=0)
    odd = 2 * np.arange(depth) + 1
    cosine, sine = trig(odd, np.arange(size_x), 2 * size_x)
    turns = np.zeros((grids, 2 * depth + 8, size_x))
    turns[:, :depth], turns[:, depth : 2 * depth] = cosine, sine
    centre = 2 * slab_x * np.arange(grids) + slab_x - 1
    turns[:, 2 * depth], turns[:, 2 * depth + 1] = trig(centre, np.arange(size_x), 2 * size_x)
    return basis_wide, low, table_wide, z_low, turns.astype(np.float32)


def cosine_of_turns(turns):
    nodes = 0.25 * np.cos((np.arange(400) + 0.5) * np.pi / 400)
    powers = nodes[:, None] ** (2 * np.arange(6)[None, :])
    fit = np.linalg.lstsq(powers, np.sin(TWO_PI * nodes) / nodes, rcond=None)[0]
    u = 0.25 - jnp.abs(turns)
    square = u * u
    value = jnp.full_like(square, float(fit[5]))
    for c in fit[4::-1]:
        value = value * square + float(c)
    return u * value


def pad_kernel(planes, items, size_y, ends, codes, out, origin, limit, plane_of):
    grid, grids = lax.axis_index("grid"), lax.axis_size("grid")
    upper = grid >= grids // 2
    middle = jnp.logical_and(grid >= grids // 4, grid < 3 * grids // 4)
    first = jnp.where(upper, size_y - grid * planes, grid * planes) - jnp.where(middle, size_y // 4, 0)
    sign = jnp.where(upper, -1, 1)
    lane = lax.broadcasted_iota(jnp.int32, (1, LANES), 1)
    flat = lax.broadcasted_iota(jnp.int32, (8, LANES), 0) * LANES + lax.broadcasted_iota(jnp.int32, (8, LANES), 1)

    def one_plane(k, place):
        start = jnp.where(k == 0, 0, ends[jnp.maximum(k - 1, 0)])
        end = ends[k]

        def one_row(c, carry):
            origin[place + c] = start + c * LANES
            limit[place + c] = end
            plane_of[place + c] = first + sign * k
            return carry

        count = lax.div(end - start + LANES - 1, LANES)
        lax.fori_loop(0, count, one_row, 0)
        return place + count

    used = lax.fori_loop(0, planes, one_plane, 0)

    def unused(i, carry):
        origin[i] = 0
        limit[i] = 0
        plane_of[i] = 0
        return carry

    lax.fori_loop(used, items, unused, 0)
    steps = 16

    def some_rows(i, marks):
        for u in range(steps):
            place = i * steps + u
            source = origin[place]
            row, shift = lax.shift_right_logical(source, 7), source & (LANES - 1)
            index = jnp.broadcast_to((lane + shift) & (LANES - 1), (8, LANES))
            pick = lambda r: jnp.take_along_axis(
                jnp.broadcast_to(codes[pl.ds(r, 1), :], (8, LANES)), index, axis=1, mode="promise_in_bounds"
            )[0:1]
            value = jnp.where(lane + shift < LANES, pick(row), pick(row + 1))
            out[pl.ds(place, 1), :] = jnp.where(source + lane < limit[place], value, -1)
            marks = jnp.where(flat == place, plane_of[place], marks)
        return marks

    out[pl.ds(items, 8), :] = lax.fori_loop(0, items // steps, some_rows, jnp.zeros((8, LANES), jnp.int32))


def pad_planes(codes, ends, size_y, items):
    return pl.pallas_call(
        functools.partial(pad_kernel, ends.shape[0], items, size_y),
        out_shape=jax.ShapeDtypeStruct((items + 8, LANES), jnp.int32),
        in_specs=[pl.BlockSpec(memory_space=pltpu.SMEM), pl.BlockSpec(memory_space=pltpu.VMEM)],
        out_specs=pl.BlockSpec(memory_space=pltpu.VMEM),
        scratch_shapes=[pltpu.SMEM((items,), jnp.int32)] * 3,
        name="pad_planes",
    )(ends, codes)


def exchange_kernel(
    plan,
    occupation, widths, own, listing, positions, species, basis_wide, basis_low, table_wide, table_low, turns, out,
    store, planes_a, planes_b, part_a, part_b, box_a, box_b, lists, marks, power, heard, votes, waves, sums, atoms,
    list_send, list_recv, mark_sem, side_send, side_recv, mate_send, mate_recv, lane_send, lane_recv,
    far_send, far_recv, hand_send, hand_recv, away_send, away_recv, pass_send, pass_recv, copy_sem,
    hop_send, hop_recv, share_send, share_recv, vote_send, vote_recv,
):
    size_x, slabs, items, pieces, share, kept = plan
    band, grid = lax.axis_index("band"), lax.axis_index("grid")
    bands, grids = lax.axis_size("band"), lax.axis_size("grid")
    core, x = lax.rem(band, 2), lax.div(band, 2)
    mate, link = lax.rem(grid, 2), lax.div(grid, 2)
    links = grids // 2
    everyone = bands * grids
    me = band * grids + grid
    slab_x, size_y, size_z = own.shape[1:]
    planes, parts, boxes = (planes_a, planes_b), (part_a, part_b), (box_a, box_b)
    leads = core == mate
    grid_of = (grid, grid + 1 - 2 * mate)
    quarter = grids // 4
    height = items + 8
    rows = basis_low.shape[1] // 2
    kept_rows = size_y // 4 + 1

    def at(index):
        return {"band": lax.div(index, grids), "grid": lax.rem(index, grids)}

    barrier = pltpu.get_barrier_semaphore()

    def greet(step, carry):
        pl.semaphore_signal(barrier, inc=1, device_id=at(lax.rem(me + step, everyone)), device_id_type=MESH)
        return carry

    lax.fori_loop(1, everyone, greet, 0)
    for i in range(own.shape[0]):
        scale = jnp.sqrt(jnp.full((size_y, size_z), occupation[i], F32))

        def scale_plane(j, carry):
            store[i, j] = own[i, j] * scale
            return carry

        lax.fori_loop(0, slab_x, scale_plane, 0)
    pl.semaphore_wait(barrier, everyone - 1)

    def remote(source, target, send, recv, device):
        return pltpu.make_async_remote_copy(
            src_ref=source, dst_ref=target, send_sem=send, recv_sem=recv,
            device_id=device, device_id_type=MESH,
        )

    beside = {"band": band + 1 - 2 * core}
    across = {"grid": grid + 1 - 2 * mate}
    far = {"band": lax.rem(band + bands // 2, bands)}

    slot_of = lambda g, c: lax.rem(g + grids - jnp.where(c == 1, quarter, 3 * quarter), grids)
    middle = jnp.logical_and(grid >= quarter, grid < 3 * quarter)
    lists_here = middle == (core == 1)
    my_slot = slot_of(grid, core)

    def list_copy(slot, step):
        return remote(
            listing, lists.at[pl.ds(pl.multiple_of(slot * height, 8), height)],
            list_send.at[step - 1], list_recv.at[slot], {"grid": lax.rem(grid + step, grids)},
        )

    own_list = pltpu.make_async_copy(
        listing, lists.at[pl.ds(pl.multiple_of(my_slot * height, 8), height)], copy_sem.at[0]
    )

    @pl.when(lists_here)
    def _():
        def send(step, carry):
            list_copy(my_slot, step).start()
            return carry

        lax.fori_loop(1, grids, send, 0)
        own_list.start()

    cut = slab_x // (CUTS // 2)
    place = lambda group, slab, c: store.at[(group * 2 + slab) * 2 + c % 2, pl.ds(c // 2 * cut, cut)]
    mine = lambda c: place(0, 0, c)
    to_side = lambda c: remote(mine(c), place(1, 0, c), side_send.at[c], side_recv.at[c], beside)
    to_mate = lambda c: remote(mine(c), place(0, 1, c), mate_send.at[c], mate_recv.at[c], across)
    to_far = lambda c: remote(mine(c), place(2, 0, c), far_send.at[c], far_recv.at[c], far)
    hand_on = lambda c: remote(place(2, 0, c), place(2, 0, c), hand_send.at[c], hand_recv.at[c], beside)
    mate_side = lambda c: remote(place(0, 1, c), place(1, 1, c), lane_send.at[c], lane_recv.at[c], beside)
    mate_far = lambda c: remote(place(0, 1, c), place(2, 1, c), away_send.at[c], away_recv.at[c], far)
    mate_hand = lambda c: remote(place(2, 1, c), place(2, 1, c), pass_send.at[c], pass_recv.at[c], beside)
    for c in range(CUTS):
        to_side(c).start()
        to_mate(c).start()

    @pl.when(leads)
    def _():
        for c in range(CUTS):
            to_far(c).start()

    def relay_far(c):
        @pl.when(leads)
        def _():
            to_far(c).wait_recv()
            hand_on(c).start()

    def relay_mate(c):
        to_mate(c).wait_recv()
        mate_side(c).start()

        @pl.when(leads)
        def _():
            mate_far(c).start()

    def relay_mate_far(c):
        @pl.when(leads)
        def _():
            mate_far(c).wait_recv()
            mate_hand(c).start()

    main = jnp.where(core == lax.rem(x + mate, 2), 0, 1)
    other = 1 - main
    base_of = (
        main * 4, main * 4 + 1, other * 4 + mate, other * 4 + 1 - mate, 8, 9,
    )

    def transform(batch, slab):
        pairs, target = BATCHES[batch], planes[batch]
        width = len(pairs) * 4 * DEPTH
        half = slab_x // 2
        unroll = math.gcd(half, 4)
        pick = lambda which, p: sum(
            jnp.where(p == q, base_of[pair[which]], 0) for q, pair in enumerate(pairs)
        ) + 2 * slab
        if half < DEPTH and slab == 0:
            target[...] = jnp.zeros_like(target)

        flat = target.reshape(kept_rows * width, size_z)

        def one_pair(p, carry):
            left, right = pick(0, p), pick(1, p)
            for block in range(half // unroll):
                stack = []
                for u in range(unroll):
                    up = half + block * unroll + u
                    down = half - 1 - block * unroll - u
                    above = store[left, up] * store[right, up]
                    below = store[left, down] * store[right, down]
                    stack += [above + below, above - below]
                high, low = split(jnp.concatenate(stack, axis=1))
                along = dot(basis_wide[core], jnp.concatenate([high, low], axis=0))
                along = along + dot(basis_low[core], high)
                stack = [along[:, i * size_z : (i + 1) * size_z] for i in range(2 * unroll)]
                high, low = split(jnp.concatenate(stack, axis=0))
                both = dot(jnp.concatenate([high, low], axis=1), table_wide[...])
                both = both + dot(high, table_low[...])
                for u in range(unroll):
                    for sign in range(2):
                        begin = (2 * u + sign) * 2 * rows
                        cosine, sine = both[begin : begin + rows], both[begin + rows : begin + 2 * rows]
                        real = cosine[:, :size_z] - sine[:, size_z:]
                        imag = -(cosine[:, size_z:] + sine[:, :size_z])
                        for part, value in ((0, real), (1, imag)):
                            row = (p * 4 + 2 * sign + part) * DEPTH + block * unroll + u
                            flat[pl.ds(row, kept_rows, stride=width), :] = value[:kept_rows]
            return carry

        lax.fori_loop(0, len(pairs), one_pair, 0)

    def code_row(t):
        slot, r = lax.div(t, items), lax.rem(t, items)
        return slot, r, lists[pl.ds(slot * height + r, 1), :]

    def mark(slot, r):
        return marks[slot * 8 + lax.shift_right_logical(r, 7), r & (LANES - 1)]

    def select(batch, slab, step):
        pairs, source, part = BATCHES[batch], planes[batch], parts[batch]
        count = len(pairs)
        first = step * (4 * RUN)
        slot = lax.div(first, items)
        r = lax.rem(first, items)
        top = slot * height + r
        base = pl.multiple_of(step * (RUN * 8 * count), 8)
        for t in range(4 * RUN):
            code = lists[pl.ds(top + t, 1), :]
            k = mark(slot, r + t)
            x_of = lax.shift_right_logical(code, size_z.bit_length() - 1) & (size_x - 1)
            x_of = jnp.broadcast_to(x_of, (8, LANES))
            z_of = jnp.broadcast_to(code & (size_z - 1), (8, LANES))
            turn = lambda i: jnp.take_along_axis(
                turns[grid_of[slab], pl.ds(8 * i, 8), :], x_of, axis=1, mode="promise_in_bounds"
            )
            get = lambda i: jnp.take_along_axis(
                source[k, pl.ds(8 * i, 8), :], z_of, axis=1, mode="promise_in_bounds"
            )
            cosine, sine, phase = turn(0), turn(1), turn(2)
            phase_cos, phase_sin = phase[0:1], phase[1:2]
            for p in range(count):
                real = jnp.sum(get(4 * p) * cosine + get(4 * p + 3) * sine, axis=0, keepdims=True)
                imag = jnp.sum(get(4 * p + 1) * cosine - get(4 * p + 2) * sine, axis=0, keepdims=True)
                for which, value in (
                    (0, real * phase_cos + imag * phase_sin),
                    (4, imag * phase_cos - real * phase_sin),
                ):
                    row = pl.ds(base + (t // 4 * 8 * count + p * 8 + which + t % 4), 1)
                    part[row, :] = value if slab == 0 else part[row, :] + value

    groups = slabs * items // 4
    half_groups = groups // 2
    piece = half_groups // pieces

    begins = lambda upward: link == (0 if upward else links - 1)
    ends = lambda upward: link == (links - 1 if upward else 0)

    def hop(batch, upward, j, source):
        tall = piece * 8 * len(BATCHES[batch])
        rows_at = pl.ds(pl.multiple_of((j + (pieces if upward else 0)) * tall, 8), tall)
        sem = ((batch * 2 + (0 if upward else 1)) * pieces) + j
        step = 2 if upward else grids - 2
        return rows_at, remote(
            source.at[rows_at], boxes[batch].at[rows_at], hop_send.at[sem], hop_recv.at[sem],
            {"grid": lax.rem(grid + step, grids)},
        )

    def forward(batch, upward, j):
        at_rows, copy = hop(batch, upward, j, boxes[batch])
        copy.wait_recv()
        box, part = boxes[batch], parts[batch]
        box[at_rows] = box[at_rows] + part[at_rows]

        @pl.when(jnp.logical_not(ends(upward)))
        def _():
            copy.start()

        @pl.when(ends(upward))
        def _():
            value = box[at_rows].reshape(piece, len(BATCHES[batch]), 8, LANES)
            total = 0.0
            for p, pair in enumerate(BATCHES[batch]):
                total = total + pair[2] * value[:, p] * value[:, p]
            total = total.reshape(piece * 8, LANES)
            spot = pl.ds(pl.multiple_of(j * (piece * 8), 8), piece * 8)
            power[spot] = total if batch == 0 else power[spot] + total

    def chain_step(step):
        for upward in (True, False):
            hops = link if upward else links - 1 - link
            j = step - HOP_LAG * hops
            for batch in range(2):
                inside = jnp.logical_and(j >= batch * pieces, j < (batch + 1) * pieces)

                @pl.when(jnp.logical_and(inside, hops > 0))
                def _():
                    forward(batch, upward, j - batch * pieces)

    def wave_parts(t):
        slot, r, code = code_row(t)
        k = mark(slot, r)
        valid = code >= 0
        x_of = lax.shift_right_arithmetic(code, size_z.bit_length() - 1) & (size_x - 1)
        z_of = code & (size_z - 1)
        upper = jnp.where((slot >= quarter) == (core == 1), 1, 0)
        fold = lambda cell, size: jnp.where(cell < size // 2 + upper, cell, cell - size).astype(F32)
        kx, kz = fold(x_of, size_x), fold(z_of, size_z)
        ky = jnp.broadcast_to(k + core * (size_y // 4), (1, LANES)).astype(F32)
        gx, gy, gz = TWO_PI / size_x * kx, TWO_PI / size_y * ky, TWO_PI / size_z * kz
        square = gx * gx + gy * gy + gz * gz
        nonzero = jnp.where(square > 0, 1.0, 0.0)
        inverse = nonzero / (square + 1.0 - nonzero)
        inverse = jnp.where(valid, inverse, 0.0)
        return kx, ky, kz, gx, gy, gz, square, inverse

    count_atoms = atoms.shape[1]
    stride = 64

    def wave_block(values, b):
        kx, ky, kz = values[:3]
        at_atoms = pl.ds(b * stride, stride)
        turn = kx * atoms[0, at_atoms] + ky * atoms[1, at_atoms] + kz * atoms[2, at_atoms]
        turn = turn - jnp.floor(turn + 0.5)
        return jnp.exp(values[6] * atoms[3, at_atoms]) * cosine_of_turns(turn)

    near = 2 * (bands // 2) * links // 2
    my_class = x * 2 + mate
    offset = jnp.where(link < links // 2, 0, near)
    order = link * (2 * (bands // 2)) + my_class
    first_chunk = order * share

    for c in range(CUTS):
        to_side(c).wait_recv()
    for b in range(count_atoms // LANES):
        lanes_at = pl.ds(b * LANES, LANES)
        kind = species[pl.ds(b, 1), :]
        square = jnp.zeros((1, LANES), F32)
        for i in range(widths.shape[0]):
            square = jnp.where(kind == i, -0.5 * widths[i] * widths[i], square)
        lines = [positions[pl.ds(i, 1), lanes_at] for i in range(3)] + [square]
        for i, line in enumerate(lines):
            atoms[i, lanes_at] = jnp.broadcast_to(line, (LANES, LANES)).T
    transform(0, 0)

    for slot in range(slabs):
        from_here = jnp.logical_and(lists_here, my_slot == slot)

        @pl.when(jnp.logical_not(from_here))
        def _():
            list_copy(slot, 1).wait_recv()

        @pl.when(from_here)
        def _():
            own_list.wait()

    def mark_copy(slot):
        return pltpu.make_async_copy(
            lists.at[pl.ds(pl.multiple_of(slot * height + items, 8), 8)],
            marks.at[pl.ds(pl.multiple_of(slot * 8, 8), 8)], mark_sem.at[slot],
        )

    for slot in range(slabs):
        mark_copy(slot).start()
    for slot in range(slabs):
        mark_copy(slot).wait()

    def select_run(batch, slab, low, high):
        def body(step, carry):
            select(batch, slab, step)
            return carry

        lax.fori_loop(low, high, body, 0)

    spans = [groups // RUN * i // CUTS for i in range(CUTS + 1)]
    for c in range(CUTS):
        relay_far(c)
        select_run(0, 0, spans[c], spans[c + 1])
        if c < CUTS // 2:
            relay_mate(c)

    @pl.when(jnp.logical_not(leads))
    def _():
        for c in range(CUTS):
            hand_on(c).wait_recv()

    transform(1, 0)
    for c in range(CUTS):
        if c < CUTS // 2:
            relay_mate(c + CUTS // 2)
        relay_mate_far(c)
        select_run(1, 0, spans[c], spans[c + 1])

    for c in range(CUTS):
        mate_side(c).wait_recv()
    transform(0, 1)

    def keep_wave(q):
        values = wave_parts(first_chunk + q)
        for b in range(count_atoms // stride):
            waves[q, pl.ds(b * stride, stride)] = wave_block(values, b)

    each = -(-kept // pieces)

    def keep_waves(i):
        for w in range(each):
            @pl.when(i * each + w < kept)
            def _():
                keep_wave(i * each + w)

    def one_piece(batch):
        def body(i, carry):
            for upward in (True, False):
                base = (i + (pieces if upward else 0)) * (piece // RUN)
                select_run(batch, 1, base, base + piece // RUN)

                @pl.when(begins(upward))
                def _():
                    hop(batch, upward, i, parts[batch])[1].start()

            chain_step(i + batch * pieces)
            if batch == 1:
                keep_waves(i)
            return carry

        return body

    lax.fori_loop(0, pieces, one_piece(0), 0)

    @pl.when(jnp.logical_not(leads))
    def _():
        for c in range(CUTS):
            mate_hand(c).wait_recv()

    transform(1, 1)
    lax.fori_loop(0, pieces, one_piece(1), 0)

    def run_out(step, carry):
        chain_step(step)
        return carry

    last = 2 * pieces
    lax.fori_loop(last, last + HOP_LAG * (links - 1), run_out, 0)

    owner = jnp.logical_or(link == 0, link == links - 1)

    def member(index):
        at_link, at_class = lax.div(index, 2 * (bands // 2)), lax.rem(index, 2 * (bands // 2))
        return {"band": lax.div(at_class, 2) * 2 + core, "grid": at_link * 2 + lax.rem(at_class, 2)}

    tall = share * 2

    def deliver(index):
        return remote(
            power.at[pl.ds(pl.multiple_of(index * tall, 8), tall)], heard.at[my_class],
            share_send.at[index], share_recv.at[my_class], member(index + offset),
        )

    @pl.when(owner)
    def _():
        def send(index, carry):
            @pl.when(index + offset != order)
            def _():
                deliver(index).start()
            return carry

        lax.fori_loop(0, near, send, 0)
        heard[my_class] = power[pl.ds(pl.multiple_of((order - offset) * tall, 8), tall)]

    for sender in range(2 * (bands // 2)):
        @pl.when(jnp.logical_not(jnp.logical_and(owner, my_class == sender)))
        def _():
            remote(
                power.at[pl.ds(0, tall)], heard.at[sender], share_send.at[0], share_recv.at[sender],
                {"grid": lax.rem(grid + 2, grids)},
            ).wait_recv()

    total = heard[0]
    for sender in range(1, 2 * (bands // 2)):
        total = total + heard[sender]
    heard[0] = total

    zero = jnp.zeros((1, LANES), F32)

    def weigh(stored):
        def body(q, carry):
            sums, stress = carry
            values = wave_parts(first_chunk + q)
            gx, gy, gz, inverse = values[3], values[4], values[5], values[7]
            row = lax.div(q, 4) * 8 + lax.rem(q, 4)
            selected = heard[0, pl.ds(row, 1), :] + heard[0, pl.ds(row + 4, 1), :]
            weighted = selected * (4.0 * math.pi) * inverse
            reduced = 2.0 * weighted * inverse
            terms = (
                weighted, reduced * gx * gx, reduced * gy * gy, reduced * gz * gz,
                reduced * gx * gy, reduced * gx * gz, reduced * gy * gz,
            )
            stress = tuple(a + b for a, b in zip(stress, terms))
            for b in range(count_atoms // stride):
                where = pl.ds(b * stride, stride)
                wave = waves[q, where] if stored else wave_block(values, b)
                sums[where] = sums[where] + weighted * wave
            return sums, stress

        return body

    def weigh_all(stored, low, high, stress, sums):
        def body(q, stress):
            return weigh(stored)(q, (sums, stress))[1]

        return lax.fori_loop(low, high, body, stress)

    sums[...] = jnp.zeros((count_atoms, LANES), F32)
    stress = weigh_all(True, 0, kept, (zero,) * 7, sums)
    if kept < share:
        stress = weigh_all(False, kept, share, stress, sums)
    blocks = []
    for b in range(count_atoms // LANES):
        blocks.append(jnp.sum(sums[pl.ds(b * LANES, LANES)].T, axis=0, keepdims=True))
    ballot = jnp.concatenate(blocks + list(stress), axis=0)
    out[...] = jnp.zeros_like(out)
    out[pl.ds(0, ballot.shape[0])] = ballot

    def vote(step):
        return remote(
            out, votes.at[me], vote_send.at[step - 1], vote_recv.at[step - 1],
            at(lax.rem(me + step, everyone)),
        )

    def cast(step, carry):
        vote(step).start()
        return carry

    def count_votes(step, carry):
        vote(step).wait_recv()
        return carry

    def settle(step, carry):
        vote(step).wait_send()
        return carry

    lax.fori_loop(1, everyone, cast, 0)
    votes[me] = out[...]

    for c in range(CUTS):
        to_side(c).wait_send()
        to_mate(c).wait_send()
        mate_side(c).wait_send()

        @pl.when(leads)
        def _():
            to_far(c).wait_send()
            hand_on(c).wait_send()
            mate_far(c).wait_send()
            mate_hand(c).wait_send()

    @pl.when(lists_here)
    def _():
        def sent(step, carry):
            list_copy(my_slot, step).wait_send()
            return carry

        lax.fori_loop(1, grids, sent, 0)

    for batch in range(2):
        def drain(j, carry):
            for upward in (True, False):
                @pl.when(jnp.logical_not(ends(upward)))
                def _():
                    hop(batch, upward, j, boxes[batch])[1].wait_send()
            return carry

        lax.fori_loop(0, pieces, drain, 0)

    @pl.when(owner)
    def _():
        def finish(index, carry):
            @pl.when(index + offset != order)
            def _():
                deliver(index).wait_send()
            return carry

        lax.fori_loop(0, near, finish, 0)

    lax.fori_loop(1, everyone, count_votes, 0)
    lax.fori_loop(1, everyone, settle, 0)
    result = votes[0]
    result = lax.fori_loop(1, everyone, lambda i, total: total + votes[i], result)
    result = result * (1.0 / (own.shape[0] * bands))
    first_row = count_atoms // LANES
    lines = jnp.sum(result, axis=1, keepdims=True)
    total, xx, yy, zz, xy, xz, yz = [lines[first_row + i : first_row + i + 1] for i in range(7)]
    lane = lax.broadcasted_iota(jnp.int32, (1, LANES), 1)
    row = jnp.zeros((1, LANES), F32)
    for i, value in enumerate((xx - total, xy, xz, xy, yy - total, yz, xz, yz, zz - total)):
        row = jnp.where(lane == i, value, row)
    out[...] = result
    out[pl.ds(first_row, 1)] = row


def exchange(own, occupation, listing, positions, species, widths, tables, turns, size_x, slabs, items):
    bands, grids = lax.axis_size("band"), lax.axis_size("grid")
    links, everyone = grids // 2, bands * grids
    pair, slab_x, size_y, size_z = own.shape
    groups = slabs * items // 4
    pieces = math.gcd(groups // 2, 12)
    near = 2 * (bands // 2) * links // 2
    share = slabs * items // 2 // near
    assert share % 4 == 0 and groups % 2 == 0
    assert groups // 2 // pieces % RUN == 0 and items % (4 * RUN) == 0
    counts = [len(b) for b in BATCHES]
    kept_rows = size_y // 4 + 1
    count_atoms = positions.shape[1]
    mib = 1024 * 1024
    used = 4 * LANES * (
        6 * pair * slab_x * size_y + kept_rows * sum(counts) * 4 * DEPTH + 2 * groups * 8 * sum(counts)
        + slabs * (items + 8) + groups * 4 + 4 * share * 2 + everyone * 16
        + pair * slab_x * size_y + 5 * count_atoms + 4000
    )
    kept = max(0, min(share, (VMEM_LIMIT - 3 * mib - used) // (4 * LANES * count_atoms)))
    plan = (size_x, slabs, items, pieces, share, kept)
    vmem = pl.BlockSpec(memory_space=pltpu.VMEM)
    dma = lambda n: pltpu.SemaphoreType.DMA((n,))
    cut = lambda: dma(CUTS)
    ins = [occupation, widths, own, listing, positions, species.reshape(-1, LANES), *tables, turns]
    smem = pl.BlockSpec(memory_space=pltpu.SMEM)
    return pl.pallas_call(
        functools.partial(exchange_kernel, plan),
        out_shape=jax.ShapeDtypeStruct((16, LANES), F32),
        in_specs=[smem] * 2 + [vmem] * (len(ins) - 2),
        out_specs=vmem,
        scratch_shapes=[
            pltpu.VMEM((6 * pair, slab_x, size_y, size_z), F32),
            *[pltpu.VMEM((kept_rows, n * 4 * DEPTH, size_z), F32) for n in counts],
            *[pltpu.VMEM((groups * 8 * n, LANES), F32) for n in counts],
            *[pltpu.VMEM((groups * 8 * n, LANES), F32) for n in counts],
            pltpu.VMEM((slabs * (items + 8), LANES), jnp.int32),
            pltpu.SMEM((slabs * 8, LANES), jnp.int32),
            pltpu.VMEM((groups // 2 * 8, LANES), F32),
            pltpu.VMEM((2 * (bands // 2), share * 2, LANES), F32),
            pltpu.VMEM((everyone, 16, LANES), F32),
            pltpu.VMEM((max(kept, 1), count_atoms, LANES), F32),
            pltpu.VMEM((count_atoms, LANES), F32),
            pltpu.VMEM((4, count_atoms, LANES), F32),
            dma(grids - 1), dma(slabs), dma(slabs),
            cut(), cut(), cut(), cut(), cut(), cut(), cut(), cut(),
            cut(), cut(), cut(), cut(), cut(), cut(), dma(1),
            dma(4 * pieces), dma(4 * pieces),
            dma(near), dma(2 * (bands // 2)),
            dma(everyone - 1), dma(everyone - 1),
        ],
        compiler_params=pltpu.CompilerParams(
            collective_id=0, has_side_effects=True, vmem_limit_bytes=VMEM_LIMIT
        ),
        name="exchange",
    )(*ins)


def per_device(orbitals, occupation, g_list, positions, species, widths):
    bands, slab_x, size_y, size_z = orbitals.shape
    grids, groups = lax.axis_size("grid"), lax.axis_size("band")
    size_x = slab_x * grids
    slab_y = size_y // grids
    assert bands == 2 and groups == 4 and grids % 4 == 0 and size_z == LANES and size_x == LANES
    grid = lax.axis_index("grid")

    plane = size_x * size_z
    key = g_list // size_z % slab_y * plane + g_list // (slab_y * size_z) * size_z + g_list % size_z
    key = lax.sort(key)
    upper = grid >= grids // 2
    x_of, z_of = key // size_z % size_x, key % size_z
    x_of = jnp.where(upper, (size_x - x_of) % size_x, x_of)
    z_of = jnp.where(upper, (size_z - z_of) % size_z, z_of)
    codes = (x_of * size_z + z_of).astype(jnp.int32).reshape(-1, LANES)
    codes = jnp.pad(codes, ((0, 8), (0, 0)))
    ends = jnp.sum((key[None, :] < (jnp.arange(slab_y)[:, None] + 1) * plane).astype(jnp.int32), axis=1)
    items = g_list.shape[0] // LANES + -(-slab_y // 16) * 16
    listing = pad_planes(codes, ends.astype(jnp.int32), size_y, items)

    tables = constant_tables(slab_x, grids, size_y, size_z)
    *held, turns = [jnp.asarray(table) for table in tables]

    out = exchange(orbitals, occupation, listing, positions, species, widths, held, turns, size_x, grids // 2, items)
    rows = positions.shape[1] // LANES
    return out[rows, :9].reshape(3, 3), out[:rows].reshape(-1)


def solution(mesh):
    return jax.shard_map(
        per_device,
        mesh=mesh,
        in_specs=(P("band", "grid", None, None), P("band"), P("grid"), P(), P(), P()),
        out_specs=(P(), P()),
        check_vma=False,
    )
```

```python
import functools
import math

import jax
import jax.numpy as jnp
import numpy as np
from jax import lax
from jax.experimental import pallas as pl
from jax.experimental.pallas import tpu as pltpu
from jax.sharding import PartitionSpec as P

HIGHEST = lax.Precision.HIGHEST
MESH = pl.DeviceIdType.MESH
TWO_PI = 2.0 * math.pi
F32 = jnp.float32
BF16 = jnp.bfloat16
LANES = 128
DEPTH = 8
RUN = 6
HOP_LAG = 2
CUTS = 4
VMEM_LIMIT = 63 * 1024 * 1024

BATCHES = (
    ((0, 0, 1.0), (0, 1, 2.0), (1, 1, 1.0), (0, 2, 2.0), (1, 3, 2.0)),
    ((0, 4, 2.0), (0, 5, 2.0), (1, 4, 2.0), (1, 5, 2.0)),
)


def trig(rows, columns, length):
    angles = TWO_PI / length * (rows[:, None] * columns[None, :] % length)
    return np.cos(angles), np.sin(angles)


def halves(table):
    table = np.asarray(table, np.float32)
    high = table.astype(jnp.bfloat16)
    low = (table - high.astype(np.float32)).astype(jnp.bfloat16)
    return high, low


def split(value):
    high = value.astype(BF16)
    low = (value - high.astype(F32)).astype(BF16)
    return high, low


def dot(a, b):
    return jnp.dot(a, b, preferred_element_type=F32)


def constant_tables(slab_x, grids, size_y, size_z):
    size_x = slab_x * grids
    half = slab_x // 2
    depth = DEPTH
    assert half <= depth
    quarter = size_y // 4
    rows = -(-(quarter + 1) // 8) * 8
    cells = float(size_x) * size_y * size_z
    bases = []
    for core in range(2):
        cosine, sine = trig(quarter * core + np.arange(quarter + 1), np.arange(size_y), size_y)
        stack = np.zeros((2, rows, size_y))
        stack[0, : quarter + 1], stack[1, : quarter + 1] = cosine / cells, sine / cells
        bases.append(stack.reshape(2 * rows, size_y))
    high, low = halves(np.stack(bases))
    basis_wide = np.concatenate([high, high], axis=2)
    cosine, sine = trig(np.arange(size_z), np.arange(size_z), size_z)
    z_high, z_low = halves(np.concatenate([cosine, sine], axis=1))
    table_wide = np.concatenate([z_high, z_high], axis=0)
    odd = 2 * np.arange(depth) + 1
    cosine, sine = trig(odd, np.arange(size_x), 2 * size_x)
    turns = np.zeros((grids, 2 * depth + 8, size_x))
    turns[:, :depth], turns[:, depth : 2 * depth] = cosine, sine
    centre = 2 * slab_x * np.arange(grids) + slab_x - 1
    turns[:, 2 * depth], turns[:, 2 * depth + 1] = trig(centre, np.arange(size_x), 2 * size_x)
    return basis_wide, low, table_wide, z_low, turns.astype(np.float32)


def cosine_of_turns(turns):
    nodes = 0.25 * np.cos((np.arange(400) + 0.5) * np.pi / 400)
    powers = nodes[:, None] ** (2 * np.arange(6)[None, :])
    fit = np.linalg.lstsq(powers, np.sin(TWO_PI * nodes) / nodes, rcond=None)[0]
    u = 0.25 - jnp.abs(turns)
    square = u * u
    value = jnp.full_like(square, float(fit[5]))
    for c in fit[4::-1]:
        value = value * square + float(c)
    return u * value


def pad_kernel(planes, items, size_y, ends, codes, out, origin, limit, plane_of):
    grid, grids = lax.axis_index("grid"), lax.axis_size("grid")
    upper = grid >= grids // 2
    middle = jnp.logical_and(grid >= grids // 4, grid < 3 * grids // 4)
    first = jnp.where(upper, size_y - grid * planes, grid * planes) - jnp.where(middle, size_y // 4, 0)
    sign = jnp.where(upper, -1, 1)
    lane = lax.broadcasted_iota(jnp.int32, (1, LANES), 1)
    flat = lax.broadcasted_iota(jnp.int32, (8, LANES), 0) * LANES + lax.broadcasted_iota(jnp.int32, (8, LANES), 1)

    def one_plane(k, place):
        start = jnp.where(k == 0, 0, ends[jnp.maximum(k - 1, 0)])
        end = ends[k]

        def one_row(c, carry):
            origin[place + c] = start + c * LANES
            limit[place + c] = end
            plane_of[place + c] = first + sign * k
            return carry

        count = lax.div(end - start + LANES - 1, LANES)
        lax.fori_loop(0, count, one_row, 0)
        return place + count

    used = lax.fori_loop(0, planes, one_plane, 0)

    def unused(i, carry):
        origin[i] = 0
        limit[i] = 0
        plane_of[i] = 0
        return carry

    lax.fori_loop(used, items, unused, 0)
    steps = 16

    def some_rows(i, marks):
        for u in range(steps):
            place = i * steps + u
            source = origin[place]
            row, shift = lax.shift_right_logical(source, 7), source & (LANES - 1)
            index = jnp.broadcast_to((lane + shift) & (LANES - 1), (8, LANES))
            pick = lambda r: jnp.take_along_axis(
                jnp.broadcast_to(codes[pl.ds(r, 1), :], (8, LANES)), index, axis=1, mode="promise_in_bounds"
            )[0:1]
            value = jnp.where(lane + shift < LANES, pick(row), pick(row + 1))
            out[pl.ds(place, 1), :] = jnp.where(source + lane < limit[place], value, -1)
            marks = jnp.where(flat == place, plane_of[place], marks)
        return marks

    out[pl.ds(items, 8), :] = lax.fori_loop(0, items // steps, some_rows, jnp.zeros((8, LANES), jnp.int32))


def pad_planes(codes, ends, size_y, items):
    return pl.pallas_call(
        functools.partial(pad_kernel, ends.shape[0], items, size_y),
        out_shape=jax.ShapeDtypeStruct((items + 8, LANES), jnp.int32),
        in_specs=[pl.BlockSpec(memory_space=pltpu.SMEM), pl.BlockSpec(memory_space=pltpu.VMEM)],
        out_specs=pl.BlockSpec(memory_space=pltpu.VMEM),
        scratch_shapes=[pltpu.SMEM((items,), jnp.int32)] * 3,
        name="pad_planes",
    )(ends, codes)


def exchange_kernel(
    plan,
    occupation, widths, own, listing, positions, species, basis_wide, basis_low, table_wide, table_low, turns, out,
    store, planes_a, planes_b, part_a, part_b, box_a, box_b, lists, marks, power, heard, votes, waves, sums, atoms,
    list_send, list_recv, mark_sem, side_send, side_recv, mate_send, mate_recv, lane_send, lane_recv,
    far_send, far_recv, hand_send, hand_recv, away_send, away_recv, pass_send, pass_recv, copy_sem,
    hop_send, hop_recv, share_send, share_recv, vote_send, vote_recv,
):
    size_x, slabs, items, pieces, share, kept = plan
    band, grid = lax.axis_index("band"), lax.axis_index("grid")
    bands, grids = lax.axis_size("band"), lax.axis_size("grid")
    core, x = lax.rem(band, 2), lax.div(band, 2)
    mate, link = lax.rem(grid, 2), lax.div(grid, 2)
    links = grids // 2
    everyone = bands * grids
    me = band * grids + grid
    slab_x, size_y, size_z = own.shape[1:]
    planes, parts, boxes = (planes_a, planes_b), (part_a, part_b), (box_a, box_b)
    leads = core == mate
    grid_of = (grid, grid + 1 - 2 * mate)
    quarter = grids // 4
    height = items + 8
    rows = basis_low.shape[1] // 2
    kept_rows = size_y // 4 + 1

    def at(index):
        return {"band": lax.div(index, grids), "grid": lax.rem(index, grids)}

    barrier = pltpu.get_barrier_semaphore()

    def greet(step, carry):
        pl.semaphore_signal(barrier, inc=1, device_id=at(lax.rem(me + step, everyone)), device_id_type=MESH)
        return carry

    lax.fori_loop(1, everyone, greet, 0)
    for i in range(own.shape[0]):
        scale = jnp.sqrt(jnp.full((size_y, size_z), occupation[i], F32))

        def scale_plane(j, carry):
            store[i, j] = own[i, j] * scale
            return carry

        lax.fori_loop(0, slab_x, scale_plane, 0)
    pl.semaphore_wait(barrier, everyone - 1)

    def remote(source, target, send, recv, device):
        return pltpu.make_async_remote_copy(
            src_ref=source, dst_ref=target, send_sem=send, recv_sem=recv,
            device_id=device, device_id_type=MESH,
        )

    beside = {"band": band + 1 - 2 * core}
    across = {"grid": grid + 1 - 2 * mate}
    far = {"band": lax.rem(band + bands // 2, bands)}

    slot_of = lambda g, c: lax.rem(g + grids - jnp.where(c == 1, quarter, 3 * quarter), grids)
    middle = jnp.logical_and(grid >= quarter, grid < 3 * quarter)
    lists_here = middle == (core == 1)
    my_slot = slot_of(grid, core)

    def list_copy(slot, step):
        return remote(
            listing, lists.at[pl.ds(pl.multiple_of(slot * height, 8), height)],
            list_send.at[step - 1], list_recv.at[slot], {"grid": lax.rem(grid + step, grids)},
        )

    own_list = pltpu.make_async_copy(
        listing, lists.at[pl.ds(pl.multiple_of(my_slot * height, 8), height)], copy_sem.at[0]
    )

    @pl.when(lists_here)
    def _():
        def send(step, carry):
            list_copy(my_slot, step).start()
            return carry

        lax.fori_loop(1, grids, send, 0)
        own_list.start()

    cut = slab_x // (CUTS // 2)
    place = lambda group, slab, c: store.at[(group * 2 + slab) * 2 + c % 2, pl.ds(c // 2 * cut, cut)]
    mine = lambda c: place(0, 0, c)
    to_side = lambda c: remote(mine(c), place(1, 0, c), side_send.at[c], side_recv.at[c], beside)
    to_mate = lambda c: remote(mine(c), place(0, 1, c), mate_send.at[c], mate_recv.at[c], across)
    to_far = lambda c: remote(mine(c), place(2, 0, c), far_send.at[c], far_recv.at[c], far)
    hand_on = lambda c: remote(place(2, 0, c), place(2, 0, c), hand_send.at[c], hand_recv.at[c], beside)
    mate_side = lambda c: remote(place(0, 1, c), place(1, 1, c), lane_send.at[c], lane_recv.at[c], beside)
    mate_far = lambda c: remote(place(0, 1, c), place(2, 1, c), away_send.at[c], away_recv.at[c], far)
    mate_hand = lambda c: remote(place(2, 1, c), place(2, 1, c), pass_send.at[c], pass_recv.at[c], beside)
    for c in range(CUTS):
        to_side(c).start()
        to_mate(c).start()

    @pl.when(leads)
    def _():
        for c in range(CUTS):
            to_far(c).start()

    def relay_far(c):
        @pl.when(leads)
        def _():
            to_far(c).wait_recv()
            hand_on(c).start()

    def relay_mate(c):
        to_mate(c).wait_recv()
        mate_side(c).start()

        @pl.when(leads)
        def _():
            mate_far(c).start()

    def relay_mate_far(c):
        @pl.when(leads)
        def _():
            mate_far(c).wait_recv()
            mate_hand(c).start()

    main = jnp.where(core == lax.rem(x + mate, 2), 0, 1)
    other = 1 - main
    base_of = (
        main * 4, main * 4 + 1, other * 4 + mate, other * 4 + 1 - mate, 8, 9,
    )

    def transform(batch, slab):
        pairs, target = BATCHES[batch], planes[batch]
        width = len(pairs) * 4 * DEPTH
        half = slab_x // 2
        unroll = math.gcd(half, 4)
        pick = lambda which, p: sum(
            jnp.where(p == q, base_of[pair[which]], 0) for q, pair in enumerate(pairs)
        ) + 2 * slab
        if half < DEPTH and slab == 0:
            target[...] = jnp.zeros_like(target)

        flat = target.reshape(kept_rows * width, size_z)

        def one_pair(p, carry):
            left, right = pick(0, p), pick(1, p)
            for block in range(half // unroll):
                stack = []
                for u in range(unroll):
                    up = half + block * unroll + u
                    down = half - 1 - block * unroll - u
                    above = store[left, up] * store[right, up]
                    below = store[left, down] * store[right, down]
                    stack += [above + below, above - below]
                high, low = split(jnp.concatenate(stack, axis=1))
                along = dot(basis_wide[core], jnp.concatenate([high, low], axis=0))
                along = along + dot(basis_low[core], high)
                stack = [along[:, i * size_z : (i + 1) * size_z] for i in range(2 * unroll)]
                high, low = split(jnp.concatenate(stack, axis=0))
                both = dot(jnp.concatenate([high, low], axis=1), table_wide[...])
                both = both + dot(high, table_low[...])
                for u in range(unroll):
                    for sign in range(2):
                        begin = (2 * u + sign) * 2 * rows
                        cosine, sine = both[begin : begin + rows], both[begin + rows : begin + 2 * rows]
                        real = cosine[:, :size_z] - sine[:, size_z:]
                        imag = -(cosine[:, size_z:] + sine[:, :size_z])
                        for part, value in ((0, real), (1, imag)):
                            row = (p * 4 + 2 * sign + part) * DEPTH + block * unroll + u
                            flat[pl.ds(row, kept_rows, stride=width), :] = value[:kept_rows]
            return carry

        lax.fori_loop(0, len(pairs), one_pair, 0)

    def code_row(t):
        slot, r = lax.div(t, items), lax.rem(t, items)
        return slot, r, lists[pl.ds(slot * height + r, 1), :]

    def mark(slot, r):
        return marks[slot * 8 + lax.shift_right_logical(r, 7), r & (LANES - 1)]

    def select(batch, slab, step):
        pairs, source, part = BATCHES[batch], planes[batch], parts[batch]
        count = len(pairs)
        first = step * (4 * RUN)
        slot = lax.div(first, items)
        r = lax.rem(first, items)
        top = slot * height + r
        base = pl.multiple_of(step * (RUN * 8 * count), 8)
        for t in range(4 * RUN):
            code = lists[pl.ds(top + t, 1), :]
            k = mark(slot, r + t)
            x_of = lax.shift_right_logical(code, size_z.bit_length() - 1) & (size_x - 1)
            x_of = jnp.broadcast_to(x_of, (8, LANES))
            z_of = jnp.broadcast_to(code & (size_z - 1), (8, LANES))
            turn = lambda i: jnp.take_along_axis(
                turns[grid_of[slab], pl.ds(8 * i, 8), :], x_of, axis=1, mode="promise_in_bounds"
            )
            get = lambda i: jnp.take_along_axis(
                source[k, pl.ds(8 * i, 8), :], z_of, axis=1, mode="promise_in_bounds"
            )
            cosine, sine, phase = turn(0), turn(1), turn(2)
            phase_cos, phase_sin = phase[0:1], phase[1:2]
            for p in range(count):
                real = jnp.sum(get(4 * p) * cosine + get(4 * p + 3) * sine, axis=0, keepdims=True)
                imag = jnp.sum(get(4 * p + 1) * cosine - get(4 * p + 2) * sine, axis=0, keepdims=True)
                for which, value in (
                    (0, real * phase_cos + imag * phase_sin),
                    (4, imag * phase_cos - real * phase_sin),
                ):
                    row = pl.ds(base + (t // 4 * 8 * count + p * 8 + which + t % 4), 1)
                    part[row, :] = value if slab == 0 else part[row, :] + value

    groups = slabs * items // 4
    half_groups = groups // 2
    piece = half_groups // pieces

    begins = lambda upward: link == (0 if upward else links - 1)
    ends = lambda upward: link == (links - 1 if upward else 0)

    def hop(batch, upward, j, source):
        tall = piece * 8 * len(BATCHES[batch])
        rows_at = pl.ds(pl.multiple_of((j + (pieces if upward else 0)) * tall, 8), tall)
        sem = ((batch * 2 + (0 if upward else 1)) * pieces) + j
        step = 2 if upward else grids - 2
        return rows_at, remote(
            source.at[rows_at], boxes[batch].at[rows_at], hop_send.at[sem], hop_recv.at[sem],
            {"grid": lax.rem(grid + step, grids)},
        )

    def forward(batch, upward, j):
        at_rows, copy = hop(batch, upward, j, boxes[batch])
        copy.wait_recv()
        box, part = boxes[batch], parts[batch]
        box[at_rows] = box[at_rows] + part[at_rows]

        @pl.when(jnp.logical_not(ends(upward)))
        def _():
            copy.start()

        @pl.when(ends(upward))
        def _():
            value = box[at_rows].reshape(piece, len(BATCHES[batch]), 8, LANES)
            total = 0.0
            for p, pair in enumerate(BATCHES[batch]):
                total = total + pair[2] * value[:, p] * value[:, p]
            total = total.reshape(piece * 8, LANES)
            spot = pl.ds(pl.multiple_of(j * (piece * 8), 8), piece * 8)
            power[spot] = total if batch == 0 else power[spot] + total

    def chain_step(step):
        for upward in (True, False):
            hops = link if upward else links - 1 - link
            j = step - HOP_LAG * hops
            for batch in range(2):
                inside = jnp.logical_and(j >= batch * pieces, j < (batch + 1) * pieces)

                @pl.when(jnp.logical_and(inside, hops > 0))
                def _():
                    forward(batch, upward, j - batch * pieces)

    def wave_parts(t):
        slot, r, code = code_row(t)
        k = mark(slot, r)
        valid = code >= 0
        x_of = lax.shift_right_arithmetic(code, size_z.bit_length() - 1) & (size_x - 1)
        z_of = code & (size_z - 1)
        upper = jnp.where((slot >= quarter) == (core == 1), 1, 0)
        fold = lambda cell, size: jnp.where(cell < size // 2 + upper, cell, cell - size).astype(F32)
        kx, kz = fold(x_of, size_x), fold(z_of, size_z)
        ky = jnp.broadcast_to(k + core * (size_y // 4), (1, LANES)).astype(F32)
        gx, gy, gz = TWO_PI / size_x * kx, TWO_PI / size_y * ky, TWO_PI / size_z * kz
        square = gx * gx + gy * gy + gz * gz
        nonzero = jnp.where(square > 0, 1.0, 0.0)
        inverse = nonzero / (square + 1.0 - nonzero)
        inverse = jnp.where(valid, inverse, 0.0)
        return kx, ky, kz, gx, gy, gz, square, inverse

    count_atoms = atoms.shape[1]
    stride = 64

    def wave_block(values, b):
        kx, ky, kz = values[:3]
        at_atoms = pl.ds(b * stride, stride)
        turn = kx * atoms[0, at_atoms] + ky * atoms[1, at_atoms] + kz * atoms[2, at_atoms]
        turn = turn - jnp.floor(turn + 0.5)
        return jnp.exp(values[6] * atoms[3, at_atoms]) * cosine_of_turns(turn)

    near = 2 * (bands // 2) * links // 2
    my_class = x * 2 + mate
    offset = jnp.where(link < links // 2, 0, near)
    order = link * (2 * (bands // 2)) + my_class
    first_chunk = order * share

    for c in range(CUTS):
        to_side(c).wait_recv()
    for b in range(count_atoms // LANES):
        lanes_at = pl.ds(b * LANES, LANES)
        kind = species[pl.ds(b, 1), :]
        square = jnp.zeros((1, LANES), F32)
        for i in range(widths.shape[0]):
            square = jnp.where(kind == i, -0.5 * widths[i] * widths[i], square)
        lines = [positions[pl.ds(i, 1), lanes_at] for i in range(3)] + [square]
        for i, line in enumerate(lines):
            atoms[i, lanes_at] = jnp.broadcast_to(line, (LANES, LANES)).T
    transform(0, 0)

    for slot in range(slabs):
        from_here = jnp.logical_and(lists_here, my_slot == slot)

        @pl.when(jnp.logical_not(from_here))
        def _():
            list_copy(slot, 1).wait_recv()

        @pl.when(from_here)
        def _():
            own_list.wait()

    def mark_copy(slot):
        return pltpu.make_async_copy(
            lists.at[pl.ds(pl.multiple_of(slot * height + items, 8), 8)],
            marks.at[pl.ds(pl.multiple_of(slot * 8, 8), 8)], mark_sem.at[slot],
        )

    for slot in range(slabs):
        mark_copy(slot).start()
    for slot in range(slabs):
        mark_copy(slot).wait()

    def select_run(batch, slab, low, high):
        def body(step, carry):
            select(batch, slab, step)
            return carry

        lax.fori_loop(low, high, body, 0)

    spans = [groups // RUN * i // CUTS for i in range(CUTS + 1)]
    for c in range(CUTS):
        relay_far(c)
        select_run(0, 0, spans[c], spans[c + 1])
        if c < CUTS // 2:
            relay_mate(c)

    @pl.when(jnp.logical_not(leads))
    def _():
        for c in range(CUTS):
            hand_on(c).wait_recv()

    transform(1, 0)
    for c in range(CUTS):
        if c < CUTS // 2:
            relay_mate(c + CUTS // 2)
        relay_mate_far(c)
        select_run(1, 0, spans[c], spans[c + 1])

    for c in range(CUTS):
        mate_side(c).wait_recv()
    transform(0, 1)

    def keep_wave(q):
        values = wave_parts(first_chunk + q)
        for b in range(count_atoms // stride):
            waves[q, pl.ds(b * stride, stride)] = wave_block(values, b)

    each = -(-kept // pieces)

    def keep_waves(i):
        for w in range(each):
            @pl.when(i * each + w < kept)
            def _():
                keep_wave(i * each + w)

    def one_piece(batch):
        def body(i, carry):
            for upward in (True, False):
                base = (i + (pieces if upward else 0)) * (piece // RUN)
                select_run(batch, 1, base, base + piece // RUN)

                @pl.when(begins(upward))
                def _():
                    hop(batch, upward, i, parts[batch])[1].start()

            chain_step(i + batch * pieces)
            if batch == 1:
                keep_waves(i)
            return carry

        return body

    lax.fori_loop(0, pieces, one_piece(0), 0)

    @pl.when(jnp.logical_not(leads))
    def _():
        for c in range(CUTS):
            mate_hand(c).wait_recv()

    transform(1, 1)
    lax.fori_loop(0, pieces, one_piece(1), 0)

    def run_out(step, carry):
        chain_step(step)
        return carry

    last = 2 * pieces
    lax.fori_loop(last, last + HOP_LAG * (links - 1), run_out, 0)

    owner = jnp.logical_or(link == 0, link == links - 1)

    def member(index):
        at_link, at_class = lax.div(index, 2 * (bands // 2)), lax.rem(index, 2 * (bands // 2))
        return {"band": lax.div(at_class, 2) * 2 + core, "grid": at_link * 2 + lax.rem(at_class, 2)}

    tall = share * 2

    def deliver(index):
        return remote(
            power.at[pl.ds(pl.multiple_of(index * tall, 8), tall)], heard.at[my_class],
            share_send.at[index], share_recv.at[my_class], member(index + offset),
        )

    @pl.when(owner)
    def _():
        def send(index, carry):
            @pl.when(index + offset != order)
            def _():
                deliver(index).start()
            return carry

        lax.fori_loop(0, near, send, 0)
        heard[my_class] = power[pl.ds(pl.multiple_of((order - offset) * tall, 8), tall)]

    for sender in range(2 * (bands // 2)):
        @pl.when(jnp.logical_not(jnp.logical_and(owner, my_class == sender)))
        def _():
            remote(
                power.at[pl.ds(0, tall)], heard.at[sender], share_send.at[0], share_recv.at[sender],
                {"grid": lax.rem(grid + 2, grids)},
            ).wait_recv()

    total = heard[0]
    for sender in range(1, 2 * (bands // 2)):
        total = total + heard[sender]
    heard[0] = total

    zero = jnp.zeros((1, LANES), F32)

    def weigh(stored):
        def body(q, carry):
            sums, stress = carry
            values = wave_parts(first_chunk + q)
            gx, gy, gz, inverse = values[3], values[4], values[5], values[7]
            row = lax.div(q, 4) * 8 + lax.rem(q, 4)
            selected = heard[0, pl.ds(row, 1), :] + heard[0, pl.ds(row + 4, 1), :]
            weighted = selected * (4.0 * math.pi) * inverse
            reduced = 2.0 * weighted * inverse
            terms = (
                weighted, reduced * gx * gx, reduced * gy * gy, reduced * gz * gz,
                reduced * gx * gy, reduced * gx * gz, reduced * gy * gz,
            )
            stress = tuple(a + b for a, b in zip(stress, terms))
            for b in range(count_atoms // stride):
                where = pl.ds(b * stride, stride)
                wave = waves[q, where] if stored else wave_block(values, b)
                sums[where] = sums[where] + weighted * wave
            return sums, stress

        return body

    def weigh_all(stored, low, high, stress, sums):
        def body(q, stress):
            return weigh(stored)(q, (sums, stress))[1]

        return lax.fori_loop(low, high, body, stress)

    sums[...] = jnp.zeros((count_atoms, LANES), F32)
    stress = weigh_all(True, 0, kept, (zero,) * 7, sums)
    if kept < share:
        stress = weigh_all(False, kept, share, stress, sums)
    blocks = []
    for b in range(count_atoms // LANES):
        blocks.append(jnp.sum(sums[pl.ds(b * LANES, LANES)].T, axis=0, keepdims=True))
    total, xx, yy, zz, xy, xz, yz = [jnp.sum(line, axis=1, keepdims=True) for line in stress]
    lane = lax.broadcasted_iota(jnp.int32, (1, LANES), 1)
    row = zero
    for i, value in enumerate((xx - total, xy, xz, xy, yy - total, yz, xz, yz, zz - total)):
        row = jnp.where(lane == i, value, row)
    ballot = jnp.concatenate(blocks + [row], axis=0)
    out[...] = jnp.zeros_like(out)
    out[pl.ds(0, ballot.shape[0])] = ballot * (1.0 / (own.shape[0] * bands))

    def vote(step):
        return remote(
            out, votes.at[me], vote_send.at[step - 1], vote_recv.at[step - 1],
            at(lax.rem(me + step, everyone)),
        )

    def cast(step, carry):
        vote(step).start()
        return carry

    def count_votes(step, carry):
        vote(step).wait_recv()
        return carry

    def settle(step, carry):
        vote(step).wait_send()
        return carry

    lax.fori_loop(1, everyone, cast, 0)
    votes[me] = out[...]

    for c in range(CUTS):
        to_side(c).wait_send()
        to_mate(c).wait_send()
        mate_side(c).wait_send()

        @pl.when(leads)
        def _():
            to_far(c).wait_send()
            hand_on(c).wait_send()
            mate_far(c).wait_send()
            mate_hand(c).wait_send()

    @pl.when(lists_here)
    def _():
        def sent(step, carry):
            list_copy(my_slot, step).wait_send()
            return carry

        lax.fori_loop(1, grids, sent, 0)

    for batch in range(2):
        def drain(j, carry):
            for upward in (True, False):
                @pl.when(jnp.logical_not(ends(upward)))
                def _():
                    hop(batch, upward, j, boxes[batch])[1].wait_send()
            return carry

        lax.fori_loop(0, pieces, drain, 0)

    @pl.when(owner)
    def _():
        def finish(index, carry):
            @pl.when(index + offset != order)
            def _():
                deliver(index).wait_send()
            return carry

        lax.fori_loop(0, near, finish, 0)

    lax.fori_loop(1, everyone, count_votes, 0)
    lax.fori_loop(1, everyone, settle, 0)
    result = votes[0]
    result = lax.fori_loop(1, everyone, lambda i, total: total + votes[i], result)
    out[...] = result


def exchange(own, occupation, listing, positions, species, widths, tables, turns, size_x, slabs, items):
    bands, grids = lax.axis_size("band"), lax.axis_size("grid")
    links, everyone = grids // 2, bands * grids
    pair, slab_x, size_y, size_z = own.shape
    groups = slabs * items // 4
    pieces = math.gcd(groups // 2, 12)
    near = 2 * (bands // 2) * links // 2
    share = slabs * items // 2 // near
    assert share % 4 == 0 and groups % 2 == 0
    assert groups // 2 // pieces % RUN == 0 and items % (4 * RUN) == 0
    counts = [len(b) for b in BATCHES]
    kept_rows = size_y // 4 + 1
    count_atoms = positions.shape[1]
    height = -(-(count_atoms // LANES + 1) // 8) * 8
    mib = 1024 * 1024
    used = 4 * LANES * (
        6 * pair * slab_x * size_y + kept_rows * sum(counts) * 4 * DEPTH + 2 * groups * 8 * sum(counts)
        + slabs * (items + 8) + groups * 4 + 4 * share * 2 + everyone * height
        + pair * slab_x * size_y + 5 * count_atoms + 4000
    )
    kept = max(0, min(share, (VMEM_LIMIT - 3 * mib - used) // (4 * LANES * count_atoms)))
    plan = (size_x, slabs, items, pieces, share, kept)
    vmem = pl.BlockSpec(memory_space=pltpu.VMEM)
    dma = lambda n: pltpu.SemaphoreType.DMA((n,))
    cut = lambda: dma(CUTS)
    ins = [occupation, widths, own, listing, positions, species.reshape(-1, LANES), *tables, turns]
    smem = pl.BlockSpec(memory_space=pltpu.SMEM)
    return pl.pallas_call(
        functools.partial(exchange_kernel, plan),
        out_shape=jax.ShapeDtypeStruct((height, LANES), F32),
        in_specs=[smem] * 2 + [vmem] * (len(ins) - 2),
        out_specs=vmem,
        scratch_shapes=[
            pltpu.VMEM((6 * pair, slab_x, size_y, size_z), F32),
            *[pltpu.VMEM((kept_rows, n * 4 * DEPTH, size_z), F32) for n in counts],
            *[pltpu.VMEM((groups * 8 * n, LANES), F32) for n in counts],
            *[pltpu.VMEM((groups * 8 * n, LANES), F32) for n in counts],
            pltpu.VMEM((slabs * (items + 8), LANES), jnp.int32),
            pltpu.SMEM((slabs * 8, LANES), jnp.int32),
            pltpu.VMEM((groups // 2 * 8, LANES), F32),
            pltpu.VMEM((2 * (bands // 2), share * 2, LANES), F32),
            pltpu.VMEM((everyone, height, LANES), F32),
            pltpu.VMEM((max(kept, 1), count_atoms, LANES), F32),
            pltpu.VMEM((count_atoms, LANES), F32),
            pltpu.VMEM((4, count_atoms, LANES), F32),
            dma(grids - 1), dma(slabs), dma(slabs),
            cut(), cut(), cut(), cut(), cut(), cut(), cut(), cut(),
            cut(), cut(), cut(), cut(), cut(), cut(), dma(1),
            dma(4 * pieces), dma(4 * pieces),
            dma(near), dma(2 * (bands // 2)),
            dma(everyone - 1), dma(everyone - 1),
        ],
        compiler_params=pltpu.CompilerParams(
            collective_id=0, has_side_effects=True, vmem_limit_bytes=VMEM_LIMIT
        ),
        name="exchange",
    )(*ins)


def per_device(orbitals, occupation, g_list, positions, species, widths):
    bands, slab_x, size_y, size_z = orbitals.shape
    grids, groups = lax.axis_size("grid"), lax.axis_size("band")
    size_x = slab_x * grids
    slab_y = size_y // grids
    assert bands == 2 and groups == 4 and grids % 4 == 0 and size_z == LANES and size_x == LANES
    grid = lax.axis_index("grid")

    plane = size_x * size_z
    key = g_list // size_z % slab_y * plane + g_list // (slab_y * size_z) * size_z + g_list % size_z
    key = lax.sort(key)
    upper = grid >= grids // 2
    x_of, z_of = key // size_z % size_x, key % size_z
    x_of = jnp.where(upper, (size_x - x_of) % size_x, x_of)
    z_of = jnp.where(upper, (size_z - z_of) % size_z, z_of)
    codes = (x_of * size_z + z_of).astype(jnp.int32).reshape(-1, LANES)
    codes = jnp.pad(codes, ((0, 8), (0, 0)))
    ends = jnp.sum((key[None, :] < (jnp.arange(slab_y)[:, None] + 1) * plane).astype(jnp.int32), axis=1)
    items = g_list.shape[0] // LANES + -(-slab_y // 16) * 16
    listing = pad_planes(codes, ends.astype(jnp.int32), size_y, items)

    tables = constant_tables(slab_x, grids, size_y, size_z)
    *held, turns = [jnp.asarray(table) for table in tables]

    out = exchange(orbitals, occupation, listing, positions, species, widths, held, turns, size_x, grids // 2, items)
    rows = positions.shape[1] // LANES
    return out[rows, :9].reshape(3, 3), out[:rows].reshape(-1)


def solution(mesh):
    return jax.shard_map(
        per_device,
        mesh=mesh,
        in_specs=(P("band", "grid", None, None), P("band"), P("grid"), P(), P(), P()),
        out_specs=(P(), P()),
        check_vma=False,
    )
```
